32 devices in a mesh: owner: 8 (over z, y), rep: 4 (over x, core).
Axes of the slice: x: 2, y: 2, z: 4, core: 2. Of those that a mesh axis runs over, the one named last changes fastest.
Arguments:
- bin_blocks: int32 [8192], P(('owner', 'rep')), may hold values from 0 to 2047, as said below
- send_counts: int32 [32, 8], P(('owner', 'rep')), may hold values from 0 to 64, as said below
- voxel_index: int32 [8192, 128], P(('owner', 'rep')), may hold values from 0 to 511
- point_sdf: bfloat16 [8192, 128], P(('owner', 'rep')), may hold values from -1 to 1
- point_weight: bfloat16 [8192, 128], P(('owner', 'rep')), may hold values from 0.099609375 to 1
- point_color: bfloat16 [8192, 3, 128], P(('owner', 'rep')), may hold values from 0 to 1
- owner_table: int32 [2048], replicated, may hold values from 0 to 2047, as said below
- old_tsdf: float32 [2048, 4, 512], P(('owner', 'rep')), may hold values from -1 to 1
- old_weight: float32 [2048, 512], P(('owner', 'rep')), may hold values from 0.5 to 4
Outputs:
- new_tsdf: float32 [2048, 4, 512], P(('owner', 'rep'))
- new_weight: float32 [2048, 512], P(('owner', 'rep'))
The draws below stay inside these ranges and needn't reach their ends.
Inputs may be any that keep to these rules, and one draw needn't show every extreme that they name: `send_counts`: each row sums to 256; every row has an entry equal to 64; among the devices s with the same s mod 4 (one frame group), some owner receives 64 bins from every one of them. `owner_table`: a permutation; entry g is the owner of block g times 256 plus the block's place among that owner's blocks. `bin_blocks`: owner_table assigns the block of bin j of device s to owner p(s, j) of the first step; of the bins that one frame group sends to one owner, at most 128 have places in any one quarter of its 256 places (places q * 64 to (q + 1) * 64 - 1), and this most is reached in every frame group.
All inputs are finite; a program needn't handle non-finite values.
Results may differ from the reference program's by a relative error of at most 0.00078.
Values may be sent and summed in bfloat16 or wider, within the bound.
A program may use at most 64 MiB of HBM per device.

```python
import math
import jax
import jax.numpy as jnp
from jax import lax

BINS = 256
OWN = 256
BLK = 128
VOX = 512
CAP = 64
NBLK = 2048
TOTAL_BINS = 8192
N_OWNER = 8
N_REP = 4


def owner_order(key):
    return jax.random.permutation(jax.random.fold_in(key, 11), OWN * N_OWNER).astype(jnp.int32)


def count_rows(key):
    base_key = jax.random.fold_in(key, 23)
    hot_owners = jax.random.randint(jax.random.fold_in(key, 29), (N_REP,), 0, N_OWNER).astype(jnp.int32)
    owner_ids = jnp.arange(N_OWNER, dtype=jnp.int32)

    def one_device(device_key, device):
        key_order, key_share = jax.random.split(device_key)
        shuffled = jax.random.permutation(key_order, N_OWNER).astype(jnp.int32)
        hot = hot_owners[device % N_REP]
        where_hot = jnp.sum(jnp.where(shuffled == hot, owner_ids, 0)).astype(jnp.int32)
        first_entry = shuffled[0]
        shuffled = shuffled.at[where_hot].set(first_entry)
        shuffled = shuffled.at[0].set(hot)
        first_share = jax.random.randint(key_share, (N_OWNER // 2,), 0, CAP + 1).astype(jnp.int32)
        first_share = first_share.at[0].set(CAP)
        row_counts = jnp.zeros((N_OWNER,), jnp.int32)
        row_counts = row_counts.at[shuffled[0::2]].set(first_share)
        row_counts = row_counts.at[shuffled[1::2]].set(CAP - first_share)
        return row_counts
    device_keys = jax.random.split(base_key, N_OWNER * N_REP)
    devices = jnp.arange(N_OWNER * N_REP, dtype=jnp.int32)
    return jax.vmap(one_device)(device_keys, devices)


def draw_owner_table(key, part):
    return owner_order(key)


def draw_send_counts(key, part):
    return count_rows(key)


def draw_bin_blocks(key, part):
    row_counts = count_rows(key)
    inverse = jnp.argsort(owner_order(key)).astype(jnp.int32)
    running_end = jnp.cumsum(row_counts, axis=1)
    starts = (running_end - row_counts).astype(jnp.int32)
    bin_ids = jnp.arange(BINS, dtype=jnp.int32)
    target = jnp.sum((bin_ids[None, :, None] >= running_end[:, None, :]).astype(jnp.int32), axis=2).astype(jnp.int32)
    grid = row_counts.reshape(N_OWNER, N_REP, N_OWNER)
    before = (jnp.cumsum(grid, axis=0) - grid).reshape(N_OWNER * N_REP, N_OWNER).astype(jnp.int32)
    position = bin_ids[None, :] - jnp.take_along_axis(starts, target, axis=1)
    rank = jnp.take_along_axis(before, target, axis=1) + position
    quarter = rank % N_REP
    share = OWN // N_REP
    offset = jax.random.randint(jax.random.fold_in(key, 37), (N_OWNER * N_REP, BINS), 0, share).astype(jnp.int32)
    local_index = (quarter * share + offset).astype(jnp.int32)
    return inverse[target * OWN + local_index].reshape(-1).astype(jnp.int32)


def place_ends(result, rng, least, high):
    index_at = [jax.random.randint(jax.random.fold_in(rng, axis), (), 0, length) for axis, length in enumerate(result.shape)]
    longest = result.shape.index(max(result.shape))
    beside = index_at[:longest] + [(index_at[longest] + 1) % result.shape[longest]] + index_at[longest + 1:]
    return result.at[tuple(index_at)].set(least).at[tuple(beside)].set(high)


def shard_levels(key, extent, cuts, smallest, high):
    loudness, own = 1.0, jax.random.fold_in(key, 6)
    for dim, blocks in cuts:
        draws = jnp.exp(jax.random.uniform(jax.random.fold_in(own, dim), (blocks,), jnp.float32, smallest / len(cuts), high / len(cuts)))
        loudness = loudness * jnp.repeat(draws, extent[dim] // blocks).reshape([-1 if axis == dim else 1 for axis in range(len(extent))])
    return loudness


def setup_inputs(seed: int = 0) -> dict:
    key_list = jax.random.split(jax.random.key(seed), 10)
    bin_blocks = draw_bin_blocks(jax.random.fold_in(key_list[9], 71), 0)
    send_counts = draw_send_counts(jax.random.fold_in(key_list[9], 71), 0)
    voxel_index = place_ends(jax.random.randint(key_list[2], (TOTAL_BINS, BLK), 0, VOX), jax.random.fold_in(key_list[2], 1), 0, VOX - 1).astype(jnp.int32)
    point_sdf = jnp.clip(jax.random.uniform(key_list[3], (TOTAL_BINS, BLK), jnp.float32, -1.0, 1.0) * shard_levels(key_list[3], (TOTAL_BINS, BLK), ((0, 32),), -0.4, 0.0), -1.0, 1.0).astype(jnp.bfloat16)
    point_weight = jnp.clip(jnp.exp(math.log(1.0) - 2.306499 * jax.random.uniform(key_list[4], (TOTAL_BINS, BLK), jnp.float32) ** shard_levels(key_list[4], (TOTAL_BINS, BLK), ((0, 32),), -0.2, 0.2)), 0.099609375, 1.0).astype(jnp.bfloat16)
    point_color = jnp.clip(1.0 * jax.random.uniform(key_list[5], (TOTAL_BINS, 3, BLK), jnp.float32) ** shard_levels(key_list[5], (TOTAL_BINS, 3, BLK), ((0, 32),), -0.2, 0.2), 0.0, 1.0).astype(jnp.bfloat16)
    owner_table = draw_owner_table(jax.random.fold_in(key_list[9], 71), 0)
    old_tsdf = jnp.clip(jax.random.uniform(key_list[7], (NBLK, 4, VOX), jnp.float32, -1.0, 1.0) * shard_levels(key_list[7], (NBLK, 4, VOX), ((0, 32),), -0.4, 0.0), -1.0, 1.0)
    old_weight = jnp.clip(jnp.exp(math.log(4.0) - 2.0794415 * jax.random.uniform(key_list[8], (NBLK, VOX), jnp.float32) ** shard_levels(key_list[8], (NBLK, VOX), ((0, 32),), -0.2, 0.2)), 0.5, 4.0)
    return dict(bin_blocks=bin_blocks, send_counts=send_counts, voxel_index=voxel_index, point_sdf=point_sdf, point_weight=point_weight, point_color=point_color, owner_table=owner_table, old_tsdf=old_tsdf, old_weight=old_weight)


def reference(bin_blocks, send_counts, voxel_index, point_sdf, point_weight, point_color, owner_table, old_tsdf, old_weight):
    running_end = jnp.cumsum(send_counts, axis=1)
    bin_ids = jnp.arange(BINS, dtype=jnp.int32)
    target = jnp.sum((bin_ids[None, :, None] >= running_end[:, None, :]).astype(jnp.int32), axis=2).reshape(-1)
    local_index = (owner_table[bin_blocks] % OWN).astype(jnp.int32)
    block_index = (target * OWN + local_index).astype(jnp.int32)
    cell_index = (block_index[:, None] * VOX + voxel_index).astype(jnp.int32)
    pieces = 8

    def add_piece(sums_now, span):
        cells, weight_raw, sdf_raw, color_raw = span
        weight = weight_raw.astype(jnp.float32)
        weighted_sdf = lax.optimization_barrier((weight * sdf_raw.astype(jnp.float32)).astype(jnp.bfloat16)).astype(jnp.float32)
        weighted_color = lax.optimization_barrier((weight[:, None, :] * color_raw.astype(jnp.float32)).astype(jnp.bfloat16)).astype(jnp.float32)
        values = jnp.concatenate([weight[:, None, :], weighted_sdf[:, None, :], weighted_color], axis=1)
        flat = jnp.transpose(values, (0, 2, 1)).reshape(-1, 5)
        return sums_now.at[cells.reshape(-1)].add(flat), None

    sums_start = jnp.zeros((NBLK * VOX, 5), jnp.float32)
    spans = (cell_index.reshape(pieces, -1, BLK), point_weight.reshape(pieces, -1, BLK),
              point_sdf.reshape(pieces, -1, BLK), point_color.reshape(pieces, -1, 3, BLK))
    sums_end, _ = lax.scan(add_piece, sums_start, spans)
    sums_cell = jnp.transpose(sums_end.reshape(NBLK, VOX, 5), (0, 2, 1))
    new_weight = old_weight + sums_cell[:, 0]
    joined_sdf = (old_weight * old_tsdf[:, 0] + sums_cell[:, 1]) / new_weight
    joined_color = (old_weight[:, None, :] * old_tsdf[:, 1:] + sums_cell[:, 2:]) / new_weight[:, None, :]
    new_tsdf = jnp.concatenate([joined_sdf[:, None, :], joined_color], axis=1)
    return new_tsdf, new_weight
```

```python
import math

import jax
import jax.numpy as jnp
from jax import lax
from jax.experimental import pallas as pl
from jax.experimental.pallas import tpu as pltpu
from jax.sharding import PartitionSpec as P

OWN = 256
VA = 8
VB = 64


def accumulate(feature_list, voxels, block_rows, block_total):
    slot_count, points = voxels.shape
    group_size = math.gcd(slot_count, 128)
    group_count = slot_count // group_size
    channels = sum_channels(feature_list)
    grouped = tuple((f.reshape((group_count, group_size) + f.shape[1:]) for f in feature_list))
    voxel_groups = voxels.reshape(group_count, group_size, points)
    block_groups = jnp.maximum(block_rows, 0).reshape(group_count, group_size)
    upper_ids = jnp.arange(VA, dtype=jnp.int32)
    lower_ids = jnp.arange(VB, dtype=jnp.int32)

    def fold_group(running, pieces):
        feature_parts, voxel_rows, block_ids = pieces
        features_group = jnp.concatenate(list(feature_parts), axis=1)
        upper_part = voxel_rows // VB
        lower_part = voxel_rows % VB
        chosen = upper_part[:, None, :] == upper_ids[None, :, None]
        left_side = jnp.where(
            chosen[:, None], features_group[:, :, None, :], jnp.zeros((), jnp.bfloat16)
        )
        left_side = left_side.reshape(group_size, channels * VA, points)
        right_side = (lower_part[:, :, None] == lower_ids[None, None, :]).astype(jnp.bfloat16)
        slot_grids = jnp.einsum(
            "gkp,gpb->gkb", left_side, right_side, preferred_element_type=jnp.float32
        )
        slot_grids = slot_grids.reshape(group_size, channels, VA * VB)
        return (running.at[block_ids].add(slot_grids), None)

    running_start = jnp.zeros((block_total, channels, VA * VB), jnp.float32)
    running_end, _ = lax.scan(fold_group, running_start, (grouped, voxel_groups, block_groups))
    return running_end


def sum_channels(feature_list):
    total_channels = 0
    for member in feature_list:
        total_channels = total_channels + member.shape[1]
    return total_channels


def local(
    bin_blocks,
    send_counts,
    voxel_index,
    point_sdf,
    point_weight,
    point_color,
    owner_table,
    old_tsdf,
    old_weight,
):
    owners = lax.axis_size("owner")
    bin_count = bin_blocks.shape[0]
    capacity = 2 * bin_count // owners
    slot_count = owners * capacity
    counts = send_counts[0]
    starts = jnp.cumsum(counts) - counts
    slot_ids = jnp.arange(slot_count, dtype=jnp.int32)
    target = slot_ids // capacity
    position = slot_ids % capacity
    active = position < counts[target]
    source = jnp.clip(starts[target] + position, 0, bin_count - 1)
    blocks_sent = jnp.where(active, owner_table[bin_blocks[source]] % OWN, -1)
    weight = jnp.where(active[:, None], point_weight[source], jnp.zeros((), jnp.bfloat16))
    wide_weight = weight.astype(jnp.float32)
    weighted_sdf = (wide_weight * point_sdf[source].astype(jnp.float32)).astype(jnp.bfloat16)
    geometry = jnp.stack([weight, weighted_sdf], axis=1)
    colors = (wide_weight[:, None, :] * point_color[source].astype(jnp.float32)).astype(
        jnp.bfloat16
    )
    voxels = voxel_index[source]
    replicas = lax.axis_size("rep")
    share = OWN // replicas
    arrived_geometry, arrived_colors, arrived_voxels, arrived_blocks = (
        lax.all_to_all(geometry, "owner", split_axis=0, concat_axis=0, tiled=True),
        lax.all_to_all(colors, "owner", split_axis=0, concat_axis=0, tiled=True),
        lax.all_to_all(voxels, "owner", split_axis=0, concat_axis=0, tiled=True),
        lax.all_to_all(blocks_sent, "owner", split_axis=0, concat_axis=0, tiled=True),
    )
    quota = 2 * bin_count // replicas
    live = arrived_blocks >= 0
    quarter = jnp.where(live, arrived_blocks // share, 0)
    quarter_ids = jnp.arange(replicas, dtype=jnp.int32)
    member = (live[:, None] & (quarter[:, None] == quarter_ids[None, :])).astype(jnp.int32)
    rank = jnp.sum((jnp.cumsum(member, axis=0) - member) * member, axis=1)
    outgoing_slots = replicas * quota
    destination = jnp.where(live, quarter * quota + rank, outgoing_slots).astype(jnp.int32)
    arrived_ids = jnp.arange(arrived_blocks.shape[0], dtype=jnp.int32)
    picked = jnp.zeros((outgoing_slots,), jnp.int32).at[destination].set(arrived_ids, mode="drop")
    filled = jnp.zeros((outgoing_slots,), jnp.bool_).at[destination].set(True, mode="drop")
    send_geometry = jnp.where(
        filled[:, None, None], arrived_geometry[picked], jnp.zeros((), jnp.bfloat16)
    )
    send_colors = jnp.where(
        filled[:, None, None], arrived_colors[picked], jnp.zeros((), jnp.bfloat16)
    )
    send_voxels = arrived_voxels[picked]
    send_places = jnp.where(filled, arrived_blocks[picked] % share, -1).astype(jnp.int32)
    final_geometry, final_colors, final_voxels, final_places = (
        lax.all_to_all(send_geometry, "rep", split_axis=0, concat_axis=0, tiled=True),
        lax.all_to_all(send_colors, "rep", split_axis=0, concat_axis=0, tiled=True),
        lax.all_to_all(send_voxels, "rep", split_axis=0, concat_axis=0, tiled=True),
        lax.all_to_all(send_places, "rep", split_axis=0, concat_axis=0, tiled=True),
    )
    cell_sums = accumulate((final_geometry, final_colors), final_voxels, final_places, share)
    geometry_share = cell_sums[:, :2]
    color_share = cell_sums[:, 2:]
    new_weight = old_weight + geometry_share[:, 0]
    joined_sdf = (old_weight * old_tsdf[:, 0] + geometry_share[:, 1]) / new_weight
    joined_color = (old_weight[:, None, :] * old_tsdf[:, 1:] + color_share) / new_weight[:, None, :]
    new_tsdf = jnp.concatenate([joined_sdf[:, None, :], joined_color], axis=1)
    return (new_tsdf, new_weight)


PLANES = 6
COLORS = 3
LANES = 128
LOG = 7
UPPERS = 8
LOWERS = 64
UNROLL = 64
FAR = (4, 5, 6, 7)
NEAR = (2, 3, 1)
GROUPS = ((0,), (1,), (2,), (3,), (4,), (5,))
MESH = pl.DeviceIdType.MESH
NT = (((1,), (1,)), ((), ()))
NN = (((1,), (0,)), ((), ()))


def mirrored(index, bits):
    bit = 1
    while bit <= bits:
        if bits & bit:
            index = index + bit * (1 - 2 * lax.rem(lax.div(index, bit), 2))
        bit *= 2
    return index


def exchange_kernel(
    owners, reps, share,
    counts_hbm, bins_hbm, table_hbm, voxel_hbm, sdf_hbm, weight_hbm, color_hbm,
    feats_ref, meta_ref,
    send1, recv1, send2, final, pick2_ref, meta_send1, meta_recv1, meta_send2, meta_recv2, listed,
    s1_send, s1_recv, m1_send, m1_recv, s2_send, s2_recv, m2_send, m2_recv,
    counts_ref, bins_ref, table_ref, voxel_ref, sdf_ref, weight_ref, color_ref, load_sem,
):
    f32, bf16, i32 = jnp.float32, jnp.bfloat16, jnp.int32
    bins = voxel_ref.shape[0]
    capacity = 2 * bins // owners
    slots = owners * capacity
    quota = 2 * bins // reps
    me = lax.axis_index("owner")
    my_rep = lax.axis_index("rep")
    barrier = pltpu.get_barrier_semaphore()
    for k in FAR + NEAR:
        pl.semaphore_signal(barrier, inc=1, device_id=(mirrored(me, k), my_rep), device_id_type=MESH)
    for k in range(1, reps):
        pl.semaphore_signal(
            barrier, inc=1, device_id=(me, mirrored(my_rep, k)), device_id_type=MESH
        )

    loads = [
        pltpu.make_async_copy(source, target, load_sem.at[i])
        for i, (source, target) in enumerate(
            (
                (counts_hbm, counts_ref),
                (voxel_hbm, voxel_ref),
                (bins_hbm, bins_ref),
                (table_hbm, table_ref),
                (weight_hbm, weight_ref),
                (sdf_hbm, sdf_ref),
                (color_hbm, color_ref),
            )
        )
    ]
    for load in loads:
        load.start()

    def owner_copy(p, k):
        partner = mirrored(me, k)
        return pltpu.make_async_remote_copy(
            src_ref=send1.at[p, pl.ds(pl.multiple_of(partner * capacity, capacity), capacity)],
            dst_ref=recv1.at[p, pl.ds(pl.multiple_of(me * capacity, capacity), capacity)],
            send_sem=s1_send.at[p, k],
            recv_sem=s1_recv.at[p, k],
            device_id=(partner, my_rep),
            device_id_type=MESH,
        )

    def owner_meta(k):
        partner = mirrored(me, k)
        return pltpu.make_async_remote_copy(
            src_ref=meta_send1.at[lax.div(partner, 2)],
            dst_ref=meta_recv1.at[me],
            send_sem=m1_send.at[k],
            recv_sem=m1_recv.at[k],
            device_id=(partner, my_rep),
            device_id_type=MESH,
        )

    def quarter_rows(q):
        return pl.ds(pl.multiple_of(q * quota, quota), quota)

    def rep_copy(p, k):
        partner = mirrored(my_rep, k)
        return pltpu.make_async_remote_copy(
            src_ref=send2.at[p, quarter_rows(partner)],
            dst_ref=final.at[p, quarter_rows(my_rep)],
            send_sem=s2_send.at[p, k],
            recv_sem=s2_recv.at[p, k],
            device_id=(me, partner),
            device_id_type=MESH,
        )

    def rep_meta(k):
        partner = mirrored(my_rep, k)
        return pltpu.make_async_remote_copy(
            src_ref=meta_send2.at[partner],
            dst_ref=meta_recv2.at[my_rep],
            send_sem=m2_send.at[k],
            recv_sem=m2_recv.at[k],
            device_id=(me, partner),
            device_id_type=MESH,
        )

    lane_bin = lax.broadcasted_iota(i32, (capacity, bins), 1)
    row_slot = lax.broadcasted_iota(i32, (capacity, bins), 0)
    loads[0].wait()
    picks = []
    start = jnp.int32(0)
    for t in range(owners):
        count = counts_ref[0, t]
        hit = (lane_bin == row_slot + start) & (row_slot < count)
        picks.append(jnp.where(hit, 1.0, 0.0).astype(bf16))
        start = start + count
    pick1 = jnp.concatenate(picks, axis=0)

    inner = lax.rem(lax.div(lax.div(me, 2) + 1, 2), 2)

    def send_plane(p, data):
        send1[p] = lax.dot_general(pick1, data, NN, preferred_element_type=f32).astype(bf16)
        if p == 0:
            pl.semaphore_wait(barrier, owners + reps - 2)
        for k in FAR[:2]:
            owner_copy(p, k).start()

        @pl.when(inner == 0)
        def _():
            for k in FAR[2:]:
                owner_copy(p, k).start()

        for k in NEAR:
            owner_copy(p, k).start()

        for group in GROUPS:
            if group[-1] == p:

                @pl.when(inner == 1)
                def _():
                    for late in group:
                        for k in FAR[2:]:
                            owner_copy(late, k).start()

    loads[1].wait()
    send_plane(0, (voxel_ref[...] - 256).astype(f32).astype(bf16))

    loads[2].wait()
    loads[3].wait()
    ids = bins_ref[...]
    low = lax.broadcasted_iota(i32, (LANES, bins), 0) == (ids & (LANES - 1))
    rows = table_ref.shape[0]
    table = (table_ref[...] & (OWN - 1)).astype(f32).astype(bf16)
    looked = lax.dot_general(
        table, jnp.where(low, 1.0, 0.0).astype(bf16), NN, preferred_element_type=f32
    )
    high = lax.broadcasted_iota(i32, (rows, bins), 0) == lax.shift_right_logical(ids, LOG)
    place = jnp.sum(jnp.where(high, looked, 0.0), axis=0, keepdims=True) + 1.0
    place = jnp.broadcast_to(place, (8, bins)).astype(bf16)
    sent_places = lax.dot_general(place, pick1, NT, preferred_element_type=f32)
    for t in range(slots // LANES):
        meta_send1[t] = sent_places[:, t * LANES : (t + 1) * LANES]
    for k in FAR + NEAR:
        owner_meta(k).start()

    loads[4].wait()
    weight = weight_ref[...]
    wide = weight.astype(f32)
    send_plane(1, weight)
    loads[5].wait()
    send_plane(2, (wide * sdf_ref[...].astype(f32)).astype(bf16))
    loads[6].wait()
    for c in range(COLORS):
        send_plane(3 + c, (wide * color_ref[c].astype(f32)).astype(bf16))

    mine = pl.ds(pl.multiple_of(me * capacity, capacity), capacity)
    for p in range(PLANES):
        recv1[p, mine] = send1[p, mine]
    meta_recv1[me] = meta_send1[lax.div(me, 2)]

    before = lax.broadcasted_iota(i32, (slots, slots), 0) < lax.broadcasted_iota(
        i32, (slots, slots), 1
    )
    before = jnp.where(before, 1.0, 0.0).astype(bf16)
    for k in FAR + NEAR:
        owner_meta(k).wait()
    lane = lax.broadcasted_iota(i32, (8, LANES), 1)
    even = lax.rem(me, 2) == 0
    pieces = []
    for pair in range(owners // 2):
        first, second = meta_recv1[2 * pair], meta_recv1[2 * pair + 1]
        first = jnp.where(even, first, pltpu.roll(first, capacity, 1))
        second = jnp.where(even, pltpu.roll(second, capacity, 1), second)
        pieces.append(jnp.where(lane < capacity, first, second))
    arrived = jnp.concatenate(pieces, axis=1)
    arrived_id = arrived.astype(i32) - 1
    quarter = jnp.where(arrived_id < 0, -1, lax.div(arrived_id, share))
    member = lax.broadcasted_iota(i32, (8, slots), 0) == quarter
    ranks = lax.dot_general(
        jnp.where(member, 1.0, 0.0).astype(bf16), before, NN, preferred_element_type=f32
    )
    rank = jnp.sum(jnp.where(member, ranks, 0.0), axis=0, keepdims=True).astype(i32)
    goal = jnp.where(arrived_id[:1] < 0, -1, quarter[:1] * quota + rank)
    pick2 = jnp.where(lax.broadcasted_iota(i32, (reps * quota, slots), 0) == goal, 1.0, 0.0)
    pick2 = pick2.astype(bf16)
    pick2_ref[...] = pick2
    final_place = jnp.where(arrived_id < 0, 0, lax.rem(arrived_id, share) + 1).astype(f32).astype(bf16)
    final_place = lax.dot_general(final_place, pick2, NT, preferred_element_type=f32)
    for q in range(reps):
        meta_send2[q] = final_place[:, q * quota : (q + 1) * quota]
    for k in range(1, reps):
        rep_meta(k).start()
    meta_recv2[my_rep] = meta_send2[my_rep]

    def relay(p):
        for k in FAR + NEAR:
            owner_copy(p, k).wait_recv()
        data = recv1[p]
        for k in (2, 3, 1):
            q = quarter_rows(mirrored(my_rep, k))
            send2[p, q] = lax.dot_general(
                pick2_ref[q], data, NN, preferred_element_type=f32
            ).astype(bf16)
            rep_copy(p, k).start()
        q = quarter_rows(my_rep)
        final[p, q] = lax.dot_general(pick2_ref[q], data, NN, preferred_element_type=f32).astype(bf16)

    def land(p):
        for k in range(1, reps):
            rep_copy(p, k).wait_recv()
        data = final[p].astype(f32)
        if p > 0:
            feats_ref[pl.ds(p - 1, slots, stride=8), :] = data
        else:
            voxel = data.astype(i32) + 256
            feats_ref[pl.ds(5, slots, stride=8), :] = (voxel & (LOWERS - 1)).astype(f32)
            feats_ref[pl.ds(6, slots, stride=8), :] = lax.shift_right_logical(voxel, 6).astype(f32)

    def list_slots():
        for k in range(1, reps):
            rep_meta(k).wait()
        lane = lax.broadcasted_iota(i32, (8, LANES), 1)
        row = lax.broadcasted_iota(i32, (8, LANES), 0)
        targets, values = [], []
        start = jnp.zeros((1, 1), f32)
        for r in range(reps):
            tile = meta_recv2[r]
            live = tile[:1] > 0
            targets.append(jnp.where(live, lane[:1].astype(f32) + start, -1.0))
            values.append(
                jnp.where(row == 0, float(r), jnp.where(row == 1, lane.astype(f32), tile))
            )
            start = start + jnp.sum(jnp.where(live, 1.0, 0.0), axis=1, keepdims=True)
        target = jnp.concatenate(targets, axis=1).astype(i32)
        chosen = lax.broadcasted_iota(i32, (slots, slots), 0) == target
        found = lax.dot_general(
            jnp.concatenate(values, axis=1).astype(bf16),
            jnp.where(chosen, 1.0, 0.0).astype(bf16),
            NT, preferred_element_type=f32,
        )
        base = ((found[:1] * float(quota) + found[1:2]) * 8.0).astype(i32)
        spot = found[2:3].astype(i32)
        spot = jnp.where(spot > 0, spot - 1, share)
        groups = slots // UNROLL
        for g in range(groups):
            part = pl.ds((g * UNROLL) // LANES * LANES, LANES)
            shift = (LANES - (g * UNROLL) % LANES) % LANES
            for source, place in ((base, g), (spot, groups + g)):
                tile = source[:, part.start : part.start + LANES]
                if shift:
                    tile = pltpu.roll(jnp.broadcast_to(tile, (8, LANES)), shift, 1)[:1]
                listed[place : place + 1] = tile
        listed[2 * groups : 2 * groups + 1] = jnp.broadcast_to(start.astype(i32), (1, LANES))
        copy = pltpu.make_async_copy(listed, meta_ref, load_sem.at[0])
        copy.start()
        return copy

    copy = None
    for p in range(PLANES):
        relay(p)
        if p == 1:
            copy = list_slots()
        if p >= 2:
            land(p - 2)
    land(PLANES - 2)
    land(PLANES - 1)
    copy.wait()
    for p in range(PLANES):
        for k in FAR + NEAR:
            owner_copy(p, k).wait_send()
        for k in range(1, reps):
            rep_copy(p, k).wait_send()


def join_kernel(
    meta_ref, feats, tsdf_hbm, oldw_hbm, new_tsdf_ref, new_weight_ref, acc, tsdf_ref, oldw_ref, sems,
):
    f32, bf16, i32 = jnp.float32, jnp.bfloat16, jnp.int32
    blocks, channels, cells = tsdf_ref.shape
    planes = channels + 1
    copies = [
        pltpu.make_async_copy(tsdf_hbm, tsdf_ref, sems.at[0]),
        pltpu.make_async_copy(oldw_hbm, oldw_ref, sems.at[1]),
    ]
    copies[0].start()
    copies[1].start()
    groups = feats.shape[0] // 8 // UNROLL
    acc[...] = jnp.zeros(acc.shape, f32)
    lower_ids = lax.broadcasted_iota(i32, (LOWERS, LANES), 0).astype(f32).astype(bf16)
    upper_ids = lax.broadcasted_iota(i32, (UPPERS, LANES), 0).astype(f32)
    empty = jnp.zeros((planes * UPPERS, LANES), f32)

    @pl.loop(0, lax.div(meta_ref[2 * groups, 0] + (UNROLL - 1), UNROLL))
    def _(g):
        for u in range(0, UNROLL, 2):
            rights, lefts, places = [], [], []
            for v in range(2):
                base = meta_ref[g, u + v]
                places.append(meta_ref[groups + g, u + v])
                lower = feats[pl.ds(base + 5, 1), :].astype(bf16)
                upper = feats[pl.ds(base + 6, 1), :]
                rights.append(jnp.where(lower_ids == lower, bf16(1), bf16(0)))
                hit = upper_ids == upper
                lefts.append(
                    jnp.concatenate(
                        [jnp.where(hit, feats[pl.ds(base + c, 1), :], 0.0) for c in range(planes)],
                        axis=0,
                    )
                )
            left = jnp.concatenate(
                [
                    jnp.concatenate([lefts[0], empty], axis=0),
                    jnp.concatenate([empty, lefts[1]], axis=0),
                ],
                axis=1,
            ).astype(bf16)
            both = lax.dot_general(
                left, jnp.concatenate(rights, axis=1), NT, preferred_element_type=f32
            )
            for v in range(2):
                rows = pl.ds(0, planes * UPPERS)
                acc[places[v], :, :LOWERS] += both[v * planes * UPPERS : (v + 1) * planes * UPPERS]

    copies[0].wait()
    copies[1].wait()
    lane = lax.broadcasted_iota(i32, (8, LANES), 1)

    @pl.loop(0, blocks // 8)
    def _(b8):
        base = pl.multiple_of(b8 * 8, 8)
        for h in range(cells // LANES):
            span = slice(h * LANES, (h + 1) * LANES)
            weights = oldw_ref[pl.ds(base, 8), span]
            news = []
            for i in range(8):
                even = acc[base + i, pl.ds(2 * h, planes, stride=UPPERS), :]
                odd = acc[base + i, pl.ds(2 * h + 1, planes, stride=UPPERS), :]
                sums = jnp.where(lane[:planes] < LOWERS, even, pltpu.roll(odd, LOWERS, 1))
                weight = weights[i : i + 1]
                total = weight + sums[:1]
                news.append(total)
                new_tsdf_ref[base + i, :, span] = (
                    weight * tsdf_ref[base + i, :, span] + sums[1:]
                ) / total
            new_weight_ref[pl.ds(base, 8), span] = jnp.concatenate(news, axis=0)


def join_call(meta, feats, old_tsdf, old_weight):
    blocks, channels, cells = old_tsdf.shape
    vmem = pl.BlockSpec(memory_space=pltpu.VMEM)
    smem = pl.BlockSpec(memory_space=pltpu.SMEM)
    hbm = pl.BlockSpec(memory_space=pl.ANY)
    return pl.pallas_call(
        join_kernel,
        out_shape=(
            jax.ShapeDtypeStruct(old_tsdf.shape, jnp.float32),
            jax.ShapeDtypeStruct(old_weight.shape, jnp.float32),
        ),
        in_specs=[smem, vmem, hbm, hbm],
        out_specs=(vmem, vmem),
        scratch_shapes=[
            pltpu.VMEM((blocks + 1, (channels + 1) * UPPERS, LANES), jnp.float32),
            pltpu.VMEM(old_tsdf.shape, jnp.float32),
            pltpu.VMEM(old_weight.shape, jnp.float32),
            pltpu.SemaphoreType.DMA((2,)),
        ],
        name="join",
    )(
        pltpu.with_memory_space_constraint(meta, pltpu.SMEM),
        pltpu.with_memory_space_constraint(feats, pltpu.VMEM),
        old_tsdf,
        old_weight,
    )


def exchange_call(
    owners, reps, bin_blocks, send_counts, voxel_index, point_sdf, point_weight, point_color,
    owner_table,
):
    bins = voxel_index.shape[0]
    capacity = 2 * bins // owners
    slots = owners * capacity
    table = owner_table.reshape(-1, LANES)
    vmem = pl.BlockSpec(memory_space=pltpu.VMEM)
    smem = pl.BlockSpec(memory_space=pltpu.SMEM)
    dma = pltpu.SemaphoreType.DMA
    listing = (2 * (slots // UNROLL) + 8, LANES)
    return pl.pallas_call(
        lambda *refs: exchange_kernel(owners, reps, OWN // reps, *refs),
        out_shape=(
            pltpu.VMEM((8 * slots, LANES), jnp.float32),
            pltpu.SMEM(listing, jnp.int32),
        ),
        in_specs=[pl.BlockSpec(memory_space=pl.ANY)] * 7,
        out_specs=(vmem, smem),
        scratch_shapes=[
            pltpu.VMEM((PLANES, slots, LANES), jnp.bfloat16),
            pltpu.VMEM((PLANES, slots, LANES), jnp.bfloat16),
            pltpu.VMEM((PLANES, slots, LANES), jnp.bfloat16),
            pltpu.VMEM((PLANES, slots, LANES), jnp.bfloat16),
            pltpu.VMEM((slots, slots), jnp.bfloat16),
            pltpu.VMEM((slots // LANES, 8, LANES), jnp.float32),
            pltpu.VMEM((owners, 8, LANES), jnp.float32),
            pltpu.VMEM((reps, 8, LANES), jnp.float32),
            pltpu.VMEM((reps, 8, LANES), jnp.float32),
            pltpu.VMEM(listing, jnp.int32),
            dma((PLANES, owners)),
            dma((PLANES, owners)),
            dma((owners,)),
            dma((owners,)),
            dma((PLANES, reps)),
            dma((PLANES, reps)),
            dma((reps,)),
            dma((reps,)),
            pltpu.SMEM(send_counts.shape, jnp.int32),
            pltpu.VMEM((1, bins), jnp.int32),
            pltpu.VMEM(table.shape, jnp.int32),
            pltpu.VMEM(voxel_index.shape, jnp.int32),
            pltpu.VMEM(point_sdf.shape, jnp.bfloat16),
            pltpu.VMEM(point_weight.shape, jnp.bfloat16),
            pltpu.VMEM((COLORS, bins, LANES), jnp.bfloat16),
            dma((7,)),
        ],
        compiler_params=pltpu.CompilerParams(collective_id=0, has_side_effects=True),
        name="exchange",
    )(
        send_counts,
        bin_blocks.reshape(1, bins),
        table,
        voxel_index,
        point_sdf,
        point_weight,
        jnp.transpose(point_color, (1, 0, 2)),
    )


def joined(
    bin_blocks,
    send_counts,
    voxel_index,
    point_sdf,
    point_weight,
    point_color,
    owner_table,
    old_tsdf,
    old_weight,
):
    owners, reps = lax.axis_size("owner"), lax.axis_size("rep")
    bins, points = voxel_index.shape
    capacity = 2 * bins // owners
    quota = 2 * bins // reps
    if owners != 8 or reps != 4 or bins != 256 or points != LANES:
        return local(
            bin_blocks, send_counts, voxel_index, point_sdf, point_weight, point_color,
            owner_table, old_tsdf, old_weight,
        )
    feats, meta = exchange_call(
        owners, reps, bin_blocks, send_counts, voxel_index, point_sdf, point_weight, point_color,
        owner_table,
    )
    return join_call(meta, feats, old_tsdf, old_weight)


def solution(mesh):
    placed = (
        P(("owner", "rep")),
        P(("owner", "rep"), None),
        P(("owner", "rep"), None),
        P(("owner", "rep"), None),
        P(("owner", "rep"), None),
        P(("owner", "rep"), None, None),
        P(),
        P(("owner", "rep"), None, None),
        P(("owner", "rep"), None),
    )
    return jax.shard_map(
        joined,
        mesh=mesh,
        in_specs=placed,
        out_specs=(P(("owner", "rep"), None, None), P(("owner", "rep"), None)),
        check_vma=False,
    )
```

```python
import math

import jax
import jax.numpy as jnp
from jax import lax
from jax.experimental import pallas as pl
from jax.experimental.pallas import tpu as pltpu
from jax.sharding import PartitionSpec as P

OWN = 256
VA = 8
VB = 64


def accumulate(feature_list, voxels, block_rows, block_total):
    slot_count, points = voxels.shape
    group_size = math.gcd(slot_count, 128)
    group_count = slot_count // group_size
    channels = sum_channels(feature_list)
    grouped = tuple((f.reshape((group_count, group_size) + f.shape[1:]) for f in feature_list))
    voxel_groups = voxels.reshape(group_count, group_size, points)
    block_groups = jnp.maximum(block_rows, 0).reshape(group_count, group_size)
    upper_ids = jnp.arange(VA, dtype=jnp.int32)
    lower_ids = jnp.arange(VB, dtype=jnp.int32)

    def fold_group(running, pieces):
        feature_parts, voxel_rows, block_ids = pieces
        features_group = jnp.concatenate(list(feature_parts), axis=1)
        upper_part = voxel_rows // VB
        lower_part = voxel_rows % VB
        chosen = upper_part[:, None, :] == upper_ids[None, :, None]
        left_side = jnp.where(
            chosen[:, None], features_group[:, :, None, :], jnp.zeros((), jnp.bfloat16)
        )
        left_side = left_side.reshape(group_size, channels * VA, points)
        right_side = (lower_part[:, :, None] == lower_ids[None, None, :]).astype(jnp.bfloat16)
        slot_grids = jnp.einsum(
            "gkp,gpb->gkb", left_side, right_side, preferred_element_type=jnp.float32
        )
        slot_grids = slot_grids.reshape(group_size, channels, VA * VB)
        return (running.at[block_ids].add(slot_grids), None)

    running_start = jnp.zeros((block_total, channels, VA * VB), jnp.float32)
    running_end, _ = lax.scan(fold_group, running_start, (grouped, voxel_groups, block_groups))
    return running_end


def sum_channels(feature_list):
    total_channels = 0
    for member in feature_list:
        total_channels = total_channels + member.shape[1]
    return total_channels


def local(
    bin_blocks,
    send_counts,
    voxel_index,
    point_sdf,
    point_weight,
    point_color,
    owner_table,
    old_tsdf,
    old_weight,
):
    owners = lax.axis_size("owner")
    bin_count = bin_blocks.shape[0]
    capacity = 2 * bin_count // owners
    slot_count = owners * capacity
    counts = send_counts[0]
    starts = jnp.cumsum(counts) - counts
    slot_ids = jnp.arange(slot_count, dtype=jnp.int32)
    target = slot_ids // capacity
    position = slot_ids % capacity
    active = position < counts[target]
    source = jnp.clip(starts[target] + position, 0, bin_count - 1)
    blocks_sent = jnp.where(active, owner_table[bin_blocks[source]] % OWN, -1)
    weight = jnp.where(active[:, None], point_weight[source], jnp.zeros((), jnp.bfloat16))
    wide_weight = weight.astype(jnp.float32)
    weighted_sdf = (wide_weight * point_sdf[source].astype(jnp.float32)).astype(jnp.bfloat16)
    geometry = jnp.stack([weight, weighted_sdf], axis=1)
    colors = (wide_weight[:, None, :] * point_color[source].astype(jnp.float32)).astype(
        jnp.bfloat16
    )
    voxels = voxel_index[source]
    replicas = lax.axis_size("rep")
    share = OWN // replicas
    arrived_geometry, arrived_colors, arrived_voxels, arrived_blocks = (
        lax.all_to_all(geometry, "owner", split_axis=0, concat_axis=0, tiled=True),
        lax.all_to_all(colors, "owner", split_axis=0, concat_axis=0, tiled=True),
        lax.all_to_all(voxels, "owner", split_axis=0, concat_axis=0, tiled=True),
        lax.all_to_all(blocks_sent, "owner", split_axis=0, concat_axis=0, tiled=True),
    )
    quota = 2 * bin_count // replicas
    live = arrived_blocks >= 0
    quarter = jnp.where(live, arrived_blocks // share, 0)
    quarter_ids = jnp.arange(replicas, dtype=jnp.int32)
    member = (live[:, None] & (quarter[:, None] == quarter_ids[None, :])).astype(jnp.int32)
    rank = jnp.sum((jnp.cumsum(member, axis=0) - member) * member, axis=1)
    outgoing_slots = replicas * quota
    destination = jnp.where(live, quarter * quota + rank, outgoing_slots).astype(jnp.int32)
    arrived_ids = jnp.arange(arrived_blocks.shape[0], dtype=jnp.int32)
    picked = jnp.zeros((outgoing_slots,), jnp.int32).at[destination].set(arrived_ids, mode="drop")
    filled = jnp.zeros((outgoing_slots,), jnp.bool_).at[destination].set(True, mode="drop")
    send_geometry = jnp.where(
        filled[:, None, None], arrived_geometry[picked], jnp.zeros((), jnp.bfloat16)
    )
    send_colors = jnp.where(
        filled[:, None, None], arrived_colors[picked], jnp.zeros((), jnp.bfloat16)
    )
    send_voxels = arrived_voxels[picked]
    send_places = jnp.where(filled, arrived_blocks[picked] % share, -1).astype(jnp.int32)
    final_geometry, final_colors, final_voxels, final_places = (
        lax.all_to_all(send_geometry, "rep", split_axis=0, concat_axis=0, tiled=True),
        lax.all_to_all(send_colors, "rep", split_axis=0, concat_axis=0, tiled=True),
        lax.all_to_all(send_voxels, "rep", split_axis=0, concat_axis=0, tiled=True),
        lax.all_to_all(send_places, "rep", split_axis=0, concat_axis=0, tiled=True),
    )
    cell_sums = accumulate((final_geometry, final_colors), final_voxels, final_places, share)
    geometry_share = cell_sums[:, :2]
    color_share = cell_sums[:, 2:]
    new_weight = old_weight + geometry_share[:, 0]
    joined_sdf = (old_weight * old_tsdf[:, 0] + geometry_share[:, 1]) / new_weight
    joined_color = (old_weight[:, None, :] * old_tsdf[:, 1:] + color_share) / new_weight[:, None, :]
    new_tsdf = jnp.concatenate([joined_sdf[:, None, :], joined_color], axis=1)
    return (new_tsdf, new_weight)


PLANES = 6
COLORS = 3
LANES = 128
LOG = 7
UPPERS = 8
LOWERS = 64
UNROLL = 64
FAR = (4, 5, 6, 7)
NEAR = (2, 3, 1)
LAG = 2
MESH = pl.DeviceIdType.MESH
NT = (((1,), (1,)), ((), ()))
NN = (((1,), (0,)), ((), ()))


def mirrored(index, bits):
    bit = 1
    while bit <= bits:
        if bits & bit:
            index = index + bit * (1 - 2 * lax.rem(lax.div(index, bit), 2))
        bit *= 2
    return index


def exchange_kernel(
    owners, reps, share,
    counts_hbm, bins_hbm, table_hbm, voxel_hbm, sdf_hbm, weight_hbm, color_hbm,
    feats_ref, meta_ref,
    send1, recv1, send2, final, pick2_ref, meta_send1, meta_recv1, meta_send2, meta_recv2, listed,
    s1_send, s1_recv, m1_send, m1_recv, s2_send, s2_recv, m2_send, m2_recv,
    counts_ref, bins_ref, table_ref, voxel_ref, sdf_ref, weight_ref, color_ref, load_sem,
):
    f32, bf16, i32 = jnp.float32, jnp.bfloat16, jnp.int32
    bins = voxel_ref.shape[0]
    capacity = 2 * bins // owners
    slots = owners * capacity
    quota = 2 * bins // reps
    me = lax.axis_index("owner")
    my_rep = lax.axis_index("rep")
    barrier = pltpu.get_barrier_semaphore()
    for k in FAR + NEAR:
        pl.semaphore_signal(barrier, inc=1, device_id=(mirrored(me, k), my_rep), device_id_type=MESH)
    for k in range(1, reps):
        pl.semaphore_signal(
            barrier, inc=1, device_id=(me, mirrored(my_rep, k)), device_id_type=MESH
        )

    loads = [
        pltpu.make_async_copy(source, target, load_sem.at[i])
        for i, (source, target) in enumerate(
            (
                (counts_hbm, counts_ref),
                (voxel_hbm, voxel_ref),
                (bins_hbm, bins_ref),
                (table_hbm, table_ref),
                (weight_hbm, weight_ref),
                (sdf_hbm, sdf_ref),
                (color_hbm, color_ref),
            )
        )
    ]
    for load in loads:
        load.start()

    def owner_copy(p, partner):
        return pltpu.make_async_remote_copy(
            src_ref=send1.at[p, pl.ds(pl.multiple_of(partner * capacity, capacity), capacity)],
            dst_ref=recv1.at[p, pl.ds(pl.multiple_of(me * capacity, capacity), capacity)],
            send_sem=s1_send,
            recv_sem=s1_recv.at[p],
            device_id=(partner, my_rep),
            device_id_type=MESH,
        )

    def took(bytes_of, semaphore):
        pltpu.make_async_copy(bytes_of, bytes_of, semaphore).wait()

    def send_copy(p, partner):
        owner_copy(p, partner).start()

    def owner_meta(k):
        partner = mirrored(me, k)
        return pltpu.make_async_remote_copy(
            src_ref=meta_send1.at[lax.div(partner, 2)],
            dst_ref=meta_recv1.at[me],
            send_sem=m1_send,
            recv_sem=m1_recv,
            device_id=(partner, my_rep),
            device_id_type=MESH,
        )

    def quarter_rows(q):
        return pl.ds(pl.multiple_of(q * quota, quota), quota)

    def rep_copy(p, k):
        partner = mirrored(my_rep, k)
        return pltpu.make_async_remote_copy(
            src_ref=send2.at[p, quarter_rows(partner)],
            dst_ref=final.at[p, quarter_rows(my_rep)],
            send_sem=s2_send,
            recv_sem=s2_recv.at[p // (PLANES - 1)],
            device_id=(me, partner),
            device_id_type=MESH,
        )

    def rep_meta(k):
        partner = mirrored(my_rep, k)
        return pltpu.make_async_remote_copy(
            src_ref=meta_send2.at[partner],
            dst_ref=meta_recv2.at[my_rep],
            send_sem=m2_send,
            recv_sem=m2_recv,
            device_id=(me, partner),
            device_id_type=MESH,
        )

    lane_bin = lax.broadcasted_iota(i32, (capacity, bins), 1)
    row_slot = lax.broadcasted_iota(i32, (capacity, bins), 0)
    loads[0].wait()
    picks = []
    start = jnp.int32(0)
    for t in range(owners):
        count = counts_ref[0, t]
        hit = (lane_bin == row_slot + start) & (row_slot < count)
        picks.append(jnp.where(hit, 1.0, 0.0).astype(bf16))
        start = start + count
    pick1 = jnp.concatenate(picks, axis=0)

    half = owners // 2
    upper_half = lax.div(me, half)
    across = (1 - upper_half) * (me + half)
    far = [mirrored(across, j) for j in range(half)]
    near = [mirrored(me, k) for k in NEAR]

    def send_plane(p, data):
        send1[p] = lax.dot_general(pick1, data, NN, preferred_element_type=f32).astype(bf16)
        if p == 0:
            pl.semaphore_wait(barrier, owners + reps - 2)
        send_copy(p, far[0])
        for partner in near:
            send_copy(p, partner)
        if p == 0:
            for partner in far[1:]:
                send_copy(p, partner)
        elif p >= LAG:
            for partner in far[1:]:
                send_copy(p - LAG + 1, partner)

    loads[1].wait()
    send_plane(0, (voxel_ref[...] - 256).astype(f32).astype(bf16))

    loads[2].wait()
    loads[3].wait()
    ids = bins_ref[...]
    low = lax.broadcasted_iota(i32, (LANES, bins), 0) == (ids & (LANES - 1))
    rows = table_ref.shape[0]
    table = (table_ref[...] & (OWN - 1)).astype(f32).astype(bf16)
    looked = lax.dot_general(
        table, jnp.where(low, 1.0, 0.0).astype(bf16), NN, preferred_element_type=f32
    )
    high = lax.broadcasted_iota(i32, (rows, bins), 0) == lax.shift_right_logical(ids, LOG)
    place = jnp.sum(jnp.where(high, looked, 0.0), axis=0, keepdims=True) + 1.0
    place = jnp.broadcast_to(place, (8, bins)).astype(bf16)
    sent_places = lax.dot_general(place, pick1, NT, preferred_element_type=f32)
    for t in range(slots // LANES):
        meta_send1[t] = sent_places[:, t * LANES : (t + 1) * LANES]
    for k in FAR + NEAR:
        owner_meta(k).start()

    loads[4].wait()
    weight = weight_ref[...]
    wide = weight.astype(f32)
    send_plane(1, weight)
    loads[5].wait()
    send_plane(2, (wide * sdf_ref[...].astype(f32)).astype(bf16))
    loads[6].wait()
    for c in range(COLORS):
        send_plane(3 + c, (wide * color_ref[c].astype(f32)).astype(bf16))

    for p in range(PLANES - LAG + 1, PLANES):
        for partner in far[1:]:
            send_copy(p, partner)

    mine = pl.ds(pl.multiple_of(me * capacity, capacity), capacity)
    for p in range(PLANES):
        recv1[p, mine] = send1[p, mine]
    meta_recv1[me] = meta_send1[lax.div(me, 2)]

    before = lax.broadcasted_iota(i32, (slots, slots), 0) < lax.broadcasted_iota(
        i32, (slots, slots), 1
    )
    before = jnp.where(before, 1.0, 0.0).astype(bf16)
    took(meta_recv1.at[pl.ds(0, owners - 1)], m1_recv)
    lane = lax.broadcasted_iota(i32, (8, LANES), 1)
    even = lax.rem(me, 2) == 0
    pieces = []
    for pair in range(owners // 2):
        first, second = meta_recv1[2 * pair], meta_recv1[2 * pair + 1]
        first = jnp.where(even, first, pltpu.roll(first, capacity, 1))
        second = jnp.where(even, pltpu.roll(second, capacity, 1), second)
        pieces.append(jnp.where(lane < capacity, first, second))
    arrived = jnp.concatenate(pieces, axis=1)
    arrived_id = arrived.astype(i32) - 1
    quarter = jnp.where(arrived_id < 0, -1, lax.div(arrived_id, share))
    member = lax.broadcasted_iota(i32, (8, slots), 0) == quarter
    ranks = lax.dot_general(
        jnp.where(member, 1.0, 0.0).astype(bf16), before, NN, preferred_element_type=f32
    )
    rank = jnp.sum(jnp.where(member, ranks, 0.0), axis=0, keepdims=True).astype(i32)
    goal = jnp.where(arrived_id[:1] < 0, -1, quarter[:1] * quota + rank)
    pick2 = jnp.where(lax.broadcasted_iota(i32, (reps * quota, slots), 0) == goal, 1.0, 0.0)
    pick2 = pick2.astype(bf16)
    pick2_ref[...] = pick2
    final_place = jnp.where(arrived_id < 0, 0, lax.rem(arrived_id, share) + 1).astype(f32).astype(bf16)
    final_place = lax.dot_general(final_place, pick2, NT, preferred_element_type=f32)
    for q in range(reps):
        meta_send2[q] = final_place[:, q * quota : (q + 1) * quota]
    for k in range(1, reps):
        rep_meta(k).start()
    meta_recv2[my_rep] = meta_send2[my_rep]

    def relay(p):
        took(recv1.at[p, pl.ds(0, (owners - 1) * capacity)], s1_recv.at[p])
        send2[p] = lax.dot_general(
            pick2_ref[...], recv1[p], NN, preferred_element_type=f32
        ).astype(bf16)
        for k in (2, 3, 1):
            rep_copy(p, k).start()
        final[p, quarter_rows(my_rep)] = send2[p, quarter_rows(my_rep)]

    def land(p):
        data = final[p].astype(f32)
        if p > 0:
            feats_ref[pl.ds(p - 1, slots, stride=8), :] = data
        else:
            voxel = data.astype(i32) + 256
            feats_ref[pl.ds(5, slots, stride=8), :] = (voxel & (LOWERS - 1)).astype(f32)
            feats_ref[pl.ds(6, slots, stride=8), :] = lax.shift_right_logical(voxel, 6).astype(f32)

    def list_slots():
        took(meta_recv2.at[pl.ds(0, reps - 1)], m2_recv)
        lane = lax.broadcasted_iota(i32, (8, LANES), 1)
        row = lax.broadcasted_iota(i32, (8, LANES), 0)
        targets, values = [], []
        start = jnp.zeros((1, 1), f32)
        for r in range(reps):
            tile = meta_recv2[r]
            live = tile[:1] > 0
            targets.append(jnp.where(live, lane[:1].astype(f32) + start, -1.0))
            values.append(
                jnp.where(row == 0, float(r), jnp.where(row == 1, lane.astype(f32), tile))
            )
            start = start + jnp.sum(jnp.where(live, 1.0, 0.0), axis=1, keepdims=True)
        target = jnp.concatenate(targets, axis=1).astype(i32)
        chosen = lax.broadcasted_iota(i32, (slots, slots), 0) == target
        found = lax.dot_general(
            jnp.concatenate(values, axis=1).astype(bf16),
            jnp.where(chosen, 1.0, 0.0).astype(bf16),
            NT, preferred_element_type=f32,
        )
        base = ((found[:1] * float(quota) + found[1:2]) * 8.0).astype(i32)
        spot = found[2:3].astype(i32)
        spot = jnp.where(spot > 0, spot - 1, share)
        groups = slots // UNROLL
        for g in range(groups):
            part = pl.ds((g * UNROLL) // LANES * LANES, LANES)
            shift = (LANES - (g * UNROLL) % LANES) % LANES
            for source, place in ((base, g), (spot, groups + g)):
                tile = source[:, part.start : part.start + LANES]
                if shift:
                    tile = pltpu.roll(jnp.broadcast_to(tile, (8, LANES)), shift, 1)[:1]
                listed[place : place + 1] = tile
        listed[2 * groups : 2 * groups + 1] = jnp.broadcast_to(start.astype(i32), (1, LANES))
        copy = pltpu.make_async_copy(listed, meta_ref, load_sem.at[0])
        copy.start()
        return copy

    for p in range(PLANES):
        relay(p)
        if p == 3:
            copy = list_slots()
    copy.wait()
    took(final.at[pl.ds(0, PLANES - 1), pl.ds(0, (reps - 1) * quota)], s2_recv.at[0])
    for p in range(PLANES - 1):
        land(p)
    took(final.at[PLANES - 1, pl.ds(0, (reps - 1) * quota)], s2_recv.at[1])
    land(PLANES - 1)
    took(send1.at[:, pl.ds(0, (owners - 1) * capacity)], s1_send)
    took(send2.at[:, pl.ds(0, (reps - 1) * quota)], s2_send)
    took(meta_recv1.at[pl.ds(0, owners - 1)], m1_send)
    took(meta_recv2.at[pl.ds(0, reps - 1)], m2_send)


def join_kernel(
    meta_ref, feats, tsdf_hbm, oldw_hbm, new_tsdf_ref, new_weight_ref, acc, tsdf_ref, oldw_ref, sems,
):
    f32, bf16, i32 = jnp.float32, jnp.bfloat16, jnp.int32
    blocks, channels, cells = tsdf_ref.shape
    planes = channels + 1
    copies = [
        pltpu.make_async_copy(tsdf_hbm, tsdf_ref, sems.at[0]),
        pltpu.make_async_copy(oldw_hbm, oldw_ref, sems.at[1]),
    ]
    copies[0].start()
    copies[1].start()
    groups = feats.shape[0] // 8 // UNROLL
    acc[...] = jnp.zeros(acc.shape, f32)
    lower_ids = lax.broadcasted_iota(i32, (LOWERS, LANES), 0).astype(f32).astype(bf16)
    upper_ids = lax.broadcasted_iota(i32, (UPPERS, LANES), 0).astype(f32)
    empty = jnp.zeros((planes * UPPERS, LANES), f32)

    @pl.loop(0, lax.div(meta_ref[2 * groups, 0] + (UNROLL - 1), UNROLL))
    def _(g):
        for u in range(0, UNROLL, 2):
            rights, lefts, places = [], [], []
            for v in range(2):
                base = meta_ref[g, u + v]
                places.append(meta_ref[groups + g, u + v])
                lower = feats[pl.ds(base + 5, 1), :].astype(bf16)
                upper = feats[pl.ds(base + 6, 1), :]
                rights.append(jnp.where(lower_ids == lower, bf16(1), bf16(0)))
                hit = upper_ids == upper
                lefts.append(
                    jnp.concatenate(
                        [jnp.where(hit, feats[pl.ds(base + c, 1), :], 0.0) for c in range(planes)],
                        axis=0,
                    )
                )
            left = jnp.concatenate(
                [
                    jnp.concatenate([lefts[0], empty], axis=0),
                    jnp.concatenate([empty, lefts[1]], axis=0),
                ],
                axis=1,
            ).astype(bf16)
            both = lax.dot_general(
                left, jnp.concatenate(rights, axis=1), NT, preferred_element_type=f32
            )
            for v in range(2):
                rows = pl.ds(0, planes * UPPERS)
                acc[places[v], :, :LOWERS] += both[v * planes * UPPERS : (v + 1) * planes * UPPERS]

    copies[0].wait()
    copies[1].wait()
    lane = lax.broadcasted_iota(i32, (8, LANES), 1)

    @pl.loop(0, blocks // 8)
    def _(b8):
        base = pl.multiple_of(b8 * 8, 8)
        for h in range(cells // LANES):
            span = slice(h * LANES, (h + 1) * LANES)
            weights = oldw_ref[pl.ds(base, 8), span]
            news = []
            for i in range(8):
                even = acc[base + i, pl.ds(2 * h, planes, stride=UPPERS), :]
                odd = acc[base + i, pl.ds(2 * h + 1, planes, stride=UPPERS), :]
                sums = jnp.where(lane[:planes] < LOWERS, even, pltpu.roll(odd, LOWERS, 1))
                weight = weights[i : i + 1]
                total = weight + sums[:1]
                news.append(total)
                new_tsdf_ref[base + i, :, span] = (
                    weight * tsdf_ref[base + i, :, span] + sums[1:]
                ) / total
            new_weight_ref[pl.ds(base, 8), span] = jnp.concatenate(news, axis=0)


def join_call(meta, feats, old_tsdf, old_weight):
    blocks, channels, cells = old_tsdf.shape
    vmem = pl.BlockSpec(memory_space=pltpu.VMEM)
    smem = pl.BlockSpec(memory_space=pltpu.SMEM)
    hbm = pl.BlockSpec(memory_space=pl.ANY)
    return pl.pallas_call(
        join_kernel,
        out_shape=(
            jax.ShapeDtypeStruct(old_tsdf.shape, jnp.float32),
            jax.ShapeDtypeStruct(old_weight.shape, jnp.float32),
        ),
        in_specs=[smem, vmem, hbm, hbm],
        out_specs=(vmem, vmem),
        scratch_shapes=[
            pltpu.VMEM((blocks + 1, (channels + 1) * UPPERS, LANES), jnp.float32),
            pltpu.VMEM(old_tsdf.shape, jnp.float32),
            pltpu.VMEM(old_weight.shape, jnp.float32),
            pltpu.SemaphoreType.DMA((2,)),
        ],
        name="join",
    )(
        pltpu.with_memory_space_constraint(meta, pltpu.SMEM),
        pltpu.with_memory_space_constraint(feats, pltpu.VMEM),
        old_tsdf,
        old_weight,
    )


def exchange_call(
    owners, reps, bin_blocks, send_counts, voxel_index, point_sdf, point_weight, point_color,
    owner_table,
):
    bins = voxel_index.shape[0]
    capacity = 2 * bins // owners
    slots = owners * capacity
    table = owner_table.reshape(-1, LANES)
    vmem = pl.BlockSpec(memory_space=pltpu.VMEM)
    smem = pl.BlockSpec(memory_space=pltpu.SMEM)
    dma = pltpu.SemaphoreType.DMA
    listing = (2 * (slots // UNROLL) + 8, LANES)
    return pl.pallas_call(
        lambda *refs: exchange_kernel(owners, reps, OWN // reps, *refs),
        out_shape=(
            pltpu.VMEM((8 * slots, LANES), jnp.float32),
            pltpu.SMEM(listing, jnp.int32),
        ),
        in_specs=[pl.BlockSpec(memory_space=pl.ANY)] * 7,
        out_specs=(vmem, smem),
        scratch_shapes=[
            pltpu.VMEM((PLANES, slots, LANES), jnp.bfloat16),
            pltpu.VMEM((PLANES, slots, LANES), jnp.bfloat16),
            pltpu.VMEM((PLANES, slots, LANES), jnp.bfloat16),
            pltpu.VMEM((PLANES, slots, LANES), jnp.bfloat16),
            pltpu.VMEM((slots, slots), jnp.bfloat16),
            pltpu.VMEM((slots // LANES, 8, LANES), jnp.float32),
            pltpu.VMEM((owners, 8, LANES), jnp.float32),
            pltpu.VMEM((reps, 8, LANES), jnp.float32),
            pltpu.VMEM((reps, 8, LANES), jnp.float32),
            pltpu.VMEM(listing, jnp.int32),
            dma,
            dma((PLANES,)),
            dma,
            dma,
            dma,
            dma((2,)),
            dma,
            dma,
            pltpu.SMEM(send_counts.shape, jnp.int32),
            pltpu.VMEM((1, bins), jnp.int32),
            pltpu.VMEM(table.shape, jnp.int32),
            pltpu.VMEM(voxel_index.shape, jnp.int32),
            pltpu.VMEM(point_sdf.shape, jnp.bfloat16),
            pltpu.VMEM(point_weight.shape, jnp.bfloat16),
            pltpu.VMEM((COLORS, bins, LANES), jnp.bfloat16),
            dma((7,)),
        ],
        compiler_params=pltpu.CompilerParams(collective_id=0, has_side_effects=True),
        name="exchange",
    )(
        send_counts,
        bin_blocks.reshape(1, bins),
        table,
        voxel_index,
        point_sdf,
        point_weight,
        jnp.transpose(point_color, (1, 0, 2)),
    )


def joined(
    bin_blocks,
    send_counts,
    voxel_index,
    point_sdf,
    point_weight,
    point_color,
    owner_table,
    old_tsdf,
    old_weight,
):
    owners, reps = lax.axis_size("owner"), lax.axis_size("rep")
    bins, points = voxel_index.shape
    capacity = 2 * bins // owners
    quota = 2 * bins // reps
    if owners != 8 or reps != 4 or bins != 256 or points != LANES:
        return local(
            bin_blocks, send_counts, voxel_index, point_sdf, point_weight, point_color,
            owner_table, old_tsdf, old_weight,
        )
    feats, meta = exchange_call(
        owners, reps, bin_blocks, send_counts, voxel_index, point_sdf, point_weight, point_color,
        owner_table,
    )
    return join_call(meta, feats, old_tsdf, old_weight)


def solution(mesh):
    placed = (
        P(("owner", "rep")),
        P(("owner", "rep"), None),
        P(("owner", "rep"), None),
        P(("owner", "rep"), None),
        P(("owner", "rep"), None),
        P(("owner", "rep"), None, None),
        P(),
        P(("owner", "rep"), None, None),
        P(("owner", "rep"), None),
    )
    return jax.shard_map(
        joined,
        mesh=mesh,
        in_specs=placed,
        out_specs=(P(("owner", "rep"), None, None), P(("owner", "rep"), None)),
        check_vma=False,
    )
```

```python
import math

import jax
import jax.numpy as jnp
from jax import lax
from jax.experimental import pallas as pl
from jax.experimental.pallas import tpu as pltpu
from jax.sharding import PartitionSpec as P

OWN = 256
VA = 8
VB = 64


def accumulate(feature_list, voxels, block_rows, block_total):
    slot_count, points = voxels.shape
    group_size = math.gcd(slot_count, 128)
    group_count = slot_count // group_size
    channels = sum_channels(feature_list)
    grouped = tuple((f.reshape((group_count, group_size) + f.shape[1:]) for f in feature_list))
    voxel_groups = voxels.reshape(group_count, group_size, points)
    block_groups = jnp.maximum(block_rows, 0).reshape(group_count, group_size)
    upper_ids = jnp.arange(VA, dtype=jnp.int32)
    lower_ids = jnp.arange(VB, dtype=jnp.int32)

    def fold_group(running, pieces):
        feature_parts, voxel_rows, block_ids = pieces
        features_group = jnp.concatenate(list(feature_parts), axis=1)
        upper_part = voxel_rows // VB
        lower_part = voxel_rows % VB
        chosen = upper_part[:, None, :] == upper_ids[None, :, None]
        left_side = jnp.where(
            chosen[:, None], features_group[:, :, None, :], jnp.zeros((), jnp.bfloat16)
        )
        left_side = left_side.reshape(group_size, channels * VA, points)
        right_side = (lower_part[:, :, None] == lower_ids[None, None, :]).astype(jnp.bfloat16)
        slot_grids = jnp.einsum(
            "gkp,gpb->gkb", left_side, right_side, preferred_element_type=jnp.float32
        )
        slot_grids = slot_grids.reshape(group_size, channels, VA * VB)
        return (running.at[block_ids].add(slot_grids), None)

    running_start = jnp.zeros((block_total, channels, VA * VB), jnp.float32)
    running_end, _ = lax.scan(fold_group, running_start, (grouped, voxel_groups, block_groups))
    return running_end


def sum_channels(feature_list):
    total_channels = 0
    for member in feature_list:
        total_channels = total_channels + member.shape[1]
    return total_channels


def local(
    bin_blocks,
    send_counts,
    voxel_index,
    point_sdf,
    point_weight,
    point_color,
    owner_table,
    old_tsdf,
    old_weight,
):
    owners = lax.axis_size("owner")
    bin_count = bin_blocks.shape[0]
    capacity = 2 * bin_count // owners
    slot_count = owners * capacity
    counts = send_counts[0]
    starts = jnp.cumsum(counts) - counts
    slot_ids = jnp.arange(slot_count, dtype=jnp.int32)
    target = slot_ids // capacity
    position = slot_ids % capacity
    active = position < counts[target]
    source = jnp.clip(starts[target] + position, 0, bin_count - 1)
    blocks_sent = jnp.where(active, owner_table[bin_blocks[source]] % OWN, -1)
    weight = jnp.where(active[:, None], point_weight[source], jnp.zeros((), jnp.bfloat16))
    wide_weight = weight.astype(jnp.float32)
    weighted_sdf = (wide_weight * point_sdf[source].astype(jnp.float32)).astype(jnp.bfloat16)
    geometry = jnp.stack([weight, weighted_sdf], axis=1)
    colors = (wide_weight[:, None, :] * point_color[source].astype(jnp.float32)).astype(
        jnp.bfloat16
    )
    voxels = voxel_index[source]
    replicas = lax.axis_size("rep")
    share = OWN // replicas
    arrived_geometry, arrived_colors, arrived_voxels, arrived_blocks = (
        lax.all_to_all(geometry, "owner", split_axis=0, concat_axis=0, tiled=True),
        lax.all_to_all(colors, "owner", split_axis=0, concat_axis=0, tiled=True),
        lax.all_to_all(voxels, "owner", split_axis=0, concat_axis=0, tiled=True),
        lax.all_to_all(blocks_sent, "owner", split_axis=0, concat_axis=0, tiled=True),
    )
    quota = 2 * bin_count // replicas
    live = arrived_blocks >= 0
    quarter = jnp.where(live, arrived_blocks // share, 0)
    quarter_ids = jnp.arange(replicas, dtype=jnp.int32)
    member = (live[:, None] & (quarter[:, None] == quarter_ids[None, :])).astype(jnp.int32)
    rank = jnp.sum((jnp.cumsum(member, axis=0) - member) * member, axis=1)
    outgoing_slots = replicas * quota
    destination = jnp.where(live, quarter * quota + rank, outgoing_slots).astype(jnp.int32)
    arrived_ids = jnp.arange(arrived_blocks.shape[0], dtype=jnp.int32)
    picked = jnp.zeros((outgoing_slots,), jnp.int32).at[destination].set(arrived_ids, mode="drop")
    filled = jnp.zeros((outgoing_slots,), jnp.bool_).at[destination].set(True, mode="drop")
    send_geometry = jnp.where(
        filled[:, None, None], arrived_geometry[picked], jnp.zeros((), jnp.bfloat16)
    )
    send_colors = jnp.where(
        filled[:, None, None], arrived_colors[picked], jnp.zeros((), jnp.bfloat16)
    )
    send_voxels = arrived_voxels[picked]
    send_places = jnp.where(filled, arrived_blocks[picked] % share, -1).astype(jnp.int32)
    final_geometry, final_colors, final_voxels, final_places = (
        lax.all_to_all(send_geometry, "rep", split_axis=0, concat_axis=0, tiled=True),
        lax.all_to_all(send_colors, "rep", split_axis=0, concat_axis=0, tiled=True),
        lax.all_to_all(send_voxels, "rep", split_axis=0, concat_axis=0, tiled=True),
        lax.all_to_all(send_places, "rep", split_axis=0, concat_axis=0, tiled=True),
    )
    cell_sums = accumulate((final_geometry, final_colors), final_voxels, final_places, share)
    geometry_share = cell_sums[:, :2]
    color_share = cell_sums[:, 2:]
    new_weight = old_weight + geometry_share[:, 0]
    joined_sdf = (old_weight * old_tsdf[:, 0] + geometry_share[:, 1]) / new_weight
    joined_color = (old_weight[:, None, :] * old_tsdf[:, 1:] + color_share) / new_weight[:, None, :]
    new_tsdf = jnp.concatenate([joined_sdf[:, None, :], joined_color], axis=1)
    return (new_tsdf, new_weight)


PLANES = 6
COLORS = 3
LANES = 128
LOG = 7
UPPERS = 8
LOWERS = 64
UNROLL = 64
FAR = (4, 5, 6, 7)
NEAR = (2, 3, 1)
LAG = 2
MESH = pl.DeviceIdType.MESH
NT = (((1,), (1,)), ((), ()))
NN = (((1,), (0,)), ((), ()))


def mirrored(index, bits):
    bit = 1
    while bit <= bits:
        if bits & bit:
            index = index + bit * (1 - 2 * lax.rem(lax.div(index, bit), 2))
        bit *= 2
    return index


def exchange_kernel(
    owners, reps, share,
    counts_hbm, bins_hbm, table_hbm, voxel_hbm, sdf_hbm, weight_hbm, color_hbm,
    feats_ref, meta_ref,
    send1, recv1, send2, final, pick2_ref, meta_send1, meta_recv1, meta_send2, meta_recv2, listed,
    s1_send, s1_recv, m1_send, m1_recv, s2_send, s2_recv, m2_send, m2_recv,
    counts_ref, bins_ref, table_ref, voxel_ref, sdf_ref, weight_ref, color_ref, load_sem,
):
    f32, bf16, i32 = jnp.float32, jnp.bfloat16, jnp.int32
    bins = voxel_ref.shape[0]
    capacity = 2 * bins // owners
    slots = owners * capacity
    quota = 2 * bins // reps
    me = lax.axis_index("owner")
    my_rep = lax.axis_index("rep")
    barrier = pltpu.get_barrier_semaphore()
    for k in FAR + NEAR:
        pl.semaphore_signal(barrier, inc=1, device_id=(mirrored(me, k), my_rep), device_id_type=MESH)
    for k in range(1, reps):
        pl.semaphore_signal(
            barrier, inc=1, device_id=(me, mirrored(my_rep, k)), device_id_type=MESH
        )

    loads = [
        pltpu.make_async_copy(source, target, load_sem.at[i])
        for i, (source, target) in enumerate(
            (
                (counts_hbm, counts_ref),
                (voxel_hbm, voxel_ref),
                (bins_hbm, bins_ref),
                (table_hbm, table_ref),
                (weight_hbm, weight_ref),
                (sdf_hbm, sdf_ref),
                (color_hbm, color_ref),
            )
        )
    ]
    for load in loads:
        load.start()

    def owner_copy(p, partner):
        return pltpu.make_async_remote_copy(
            src_ref=send1.at[p, pl.ds(pl.multiple_of(partner * capacity, capacity), capacity)],
            dst_ref=recv1.at[p, pl.ds(pl.multiple_of(me * capacity, capacity), capacity)],
            send_sem=s1_send,
            recv_sem=s1_recv.at[p],
            device_id=(partner, my_rep),
            device_id_type=MESH,
        )

    def took(bytes_of, semaphore):
        pltpu.make_async_copy(bytes_of, bytes_of, semaphore).wait()

    def send_copy(p, partner):
        owner_copy(p, partner).start()

    def owner_meta(k):
        partner = mirrored(me, k)
        return pltpu.make_async_remote_copy(
            src_ref=meta_send1.at[lax.div(partner, 2)],
            dst_ref=meta_recv1.at[me],
            send_sem=m1_send,
            recv_sem=m1_recv,
            device_id=(partner, my_rep),
            device_id_type=MESH,
        )

    def quarter_rows(q):
        return pl.ds(pl.multiple_of(q * quota, quota), quota)

    def rep_copy(p, k):
        partner = mirrored(my_rep, k)
        return pltpu.make_async_remote_copy(
            src_ref=send2.at[p, quarter_rows(partner)],
            dst_ref=final.at[p, quarter_rows(my_rep)],
            send_sem=s2_send,
            recv_sem=s2_recv.at[p // (PLANES - 1)],
            device_id=(me, partner),
            device_id_type=MESH,
        )

    def rep_meta(k):
        partner = mirrored(my_rep, k)
        return pltpu.make_async_remote_copy(
            src_ref=meta_send2.at[partner],
            dst_ref=meta_recv2.at[my_rep],
            send_sem=m2_send,
            recv_sem=m2_recv,
            device_id=(me, partner),
            device_id_type=MESH,
        )

    lane_bin = lax.broadcasted_iota(i32, (capacity, bins), 1)
    row_slot = lax.broadcasted_iota(i32, (capacity, bins), 0)
    loads[0].wait()
    picks = []
    start = jnp.int32(0)
    for t in range(owners):
        count = counts_ref[0, t]
        hit = (lane_bin == row_slot + start) & (row_slot < count)
        picks.append(jnp.where(hit, 1.0, 0.0).astype(bf16))
        start = start + count
    pick1 = jnp.concatenate(picks, axis=0)

    half = owners // 2
    upper_half = lax.div(me, half)
    across = (1 - upper_half) * (me + half)
    far = [mirrored(across, j) for j in range(half)]
    near = [mirrored(me, k) for k in NEAR]

    def send_plane(p, data):
        send1[p] = lax.dot_general(pick1, data, NN, preferred_element_type=f32).astype(bf16)
        if p == 0:
            pl.semaphore_wait(barrier, owners + reps - 2)
        send_copy(p, far[0])
        for partner in near:
            send_copy(p, partner)
        if p == 0:
            for partner in far[1:]:
                send_copy(p, partner)
        elif p >= LAG:
            for partner in far[1:]:
                send_copy(p - LAG + 1, partner)

    loads[1].wait()
    send_plane(0, (voxel_ref[...] - 256).astype(f32).astype(bf16))

    loads[2].wait()
    loads[3].wait()
    ids = bins_ref[...]
    low = lax.broadcasted_iota(i32, (LANES, bins), 0) == (ids & (LANES - 1))
    rows = table_ref.shape[0]
    table = (table_ref[...] & (OWN - 1)).astype(f32).astype(bf16)
    looked = lax.dot_general(
        table, jnp.where(low, 1.0, 0.0).astype(bf16), NN, preferred_element_type=f32
    )
    high = lax.broadcasted_iota(i32, (rows, bins), 0) == lax.shift_right_logical(ids, LOG)
    place = jnp.sum(jnp.where(high, looked, 0.0), axis=0, keepdims=True) + 1.0
    place = jnp.broadcast_to(place, (8, bins)).astype(bf16)
    sent_places = lax.dot_general(place, pick1, NT, preferred_element_type=f32)
    for t in range(slots // LANES):
        meta_send1[t] = sent_places[:, t * LANES : (t + 1) * LANES]
    for k in FAR + NEAR:
        owner_meta(k).start()

    loads[4].wait()
    weight = weight_ref[...]
    wide = weight.astype(f32)
    send_plane(1, weight)
    loads[5].wait()
    send_plane(2, (wide * sdf_ref[...].astype(f32)).astype(bf16))
    loads[6].wait()
    for c in range(COLORS):
        send_plane(3 + c, (wide * color_ref[c].astype(f32)).astype(bf16))

    for p in range(PLANES - LAG + 1, PLANES):
        for partner in far[1:]:
            send_copy(p, partner)

    mine = pl.ds(pl.multiple_of(me * capacity, capacity), capacity)
    for p in range(PLANES):
        recv1[p, mine] = send1[p, mine]
    meta_recv1[me] = meta_send1[lax.div(me, 2)]

    before = lax.broadcasted_iota(i32, (slots, slots), 0) < lax.broadcasted_iota(
        i32, (slots, slots), 1
    )
    before = jnp.where(before, 1.0, 0.0).astype(bf16)
    took(meta_recv1.at[pl.ds(0, owners - 1)], m1_recv)
    lane = lax.broadcasted_iota(i32, (8, LANES), 1)
    even = lax.rem(me, 2) == 0
    pieces = []
    for pair in range(owners // 2):
        first, second = meta_recv1[2 * pair], meta_recv1[2 * pair + 1]
        first = jnp.where(even, first, pltpu.roll(first, capacity, 1))
        second = jnp.where(even, pltpu.roll(second, capacity, 1), second)
        pieces.append(jnp.where(lane < capacity, first, second))
    arrived = jnp.concatenate(pieces, axis=1)
    arrived_id = arrived.astype(i32) - 1
    quarter = jnp.where(arrived_id < 0, -1, lax.div(arrived_id, share))
    member = lax.broadcasted_iota(i32, (8, slots), 0) == quarter
    ranks = lax.dot_general(
        jnp.where(member, 1.0, 0.0).astype(bf16), before, NN, preferred_element_type=f32
    )
    rank = jnp.sum(jnp.where(member, ranks, 0.0), axis=0, keepdims=True).astype(i32)
    goal = jnp.where(arrived_id[:1] < 0, -1, quarter[:1] * quota + rank)
    pick2 = jnp.where(lax.broadcasted_iota(i32, (reps * quota, slots), 0) == goal, 1.0, 0.0)
    pick2 = pick2.astype(bf16)
    pick2_ref[...] = pick2
    final_place = jnp.where(arrived_id < 0, 0, lax.rem(arrived_id, share) + 1).astype(f32).astype(bf16)
    final_place = lax.dot_general(final_place, pick2, NT, preferred_element_type=f32)
    for q in range(reps):
        meta_send2[q] = final_place[:, q * quota : (q + 1) * quota]
    for k in range(1, reps):
        rep_meta(k).start()
    meta_recv2[my_rep] = meta_send2[my_rep]

    def relay(p):
        took(recv1.at[p, pl.ds(0, (owners - 1) * capacity)], s1_recv.at[p])
        send2[p] = lax.dot_general(
            pick2_ref[...], recv1[p], NN, preferred_element_type=f32
        ).astype(bf16)
        for k in (2, 3, 1):
            rep_copy(p, k).start()
        final[p, quarter_rows(my_rep)] = send2[p, quarter_rows(my_rep)]

    def land(p):
        data = final[p].astype(f32)
        if p > 0:
            feats_ref[pl.ds(p - 1, slots, stride=8), :] = data
        else:
            voxel = data.astype(i32) + 256
            feats_ref[pl.ds(5, slots, stride=8), :] = (voxel & (LOWERS - 1)).astype(f32)
            feats_ref[pl.ds(6, slots, stride=8), :] = lax.shift_right_logical(voxel, 6).astype(f32)

    def list_slots():
        took(meta_recv2.at[pl.ds(0, reps - 1)], m2_recv)
        lane = lax.broadcasted_iota(i32, (8, LANES), 1)
        row = lax.broadcasted_iota(i32, (8, LANES), 0)
        targets, values = [], []
        start = jnp.zeros((1, 1), f32)
        for r in range(reps):
            tile = meta_recv2[r]
            live = tile[:1] > 0
            targets.append(jnp.where(live, lane[:1].astype(f32) + start, -1.0))
            values.append(
                jnp.where(row == 0, float(r), jnp.where(row == 1, lane.astype(f32), tile))
            )
            start = start + jnp.sum(jnp.where(live, 1.0, 0.0), axis=1, keepdims=True)
        target = jnp.concatenate(targets, axis=1).astype(i32)
        chosen = lax.broadcasted_iota(i32, (slots, slots), 0) == target
        found = lax.dot_general(
            jnp.concatenate(values, axis=1).astype(bf16),
            jnp.where(chosen, 1.0, 0.0).astype(bf16),
            NT, preferred_element_type=f32,
        )
        base = ((found[:1] * float(quota) + found[1:2]) * 8.0).astype(i32)
        spot = found[2:3].astype(i32)
        spot = jnp.where(spot > 0, spot - 1, share)
        groups = slots // UNROLL
        for g in range(groups):
            part = pl.ds((g * UNROLL) // LANES * LANES, LANES)
            shift = (LANES - (g * UNROLL) % LANES) % LANES
            for source, place in ((base, g), (spot, groups + g)):
                tile = source[:, part.start : part.start + LANES]
                if shift:
                    tile = pltpu.roll(jnp.broadcast_to(tile, (8, LANES)), shift, 1)[:1]
                listed[place : place + 1] = tile
        listed[2 * groups : 2 * groups + 1] = jnp.broadcast_to(start.astype(i32), (1, LANES))
        copy = pltpu.make_async_copy(listed, meta_ref, load_sem.at[0])
        copy.start()
        return copy

    for p in range(PLANES):
        relay(p)
        if p == 3:
            copy = list_slots()
    copy.wait()
    took(final.at[pl.ds(0, PLANES - 1), pl.ds(0, (reps - 1) * quota)], s2_recv.at[0])
    for p in range(PLANES - 1):
        land(p)
    took(final.at[PLANES - 1, pl.ds(0, (reps - 1) * quota)], s2_recv.at[1])
    land(PLANES - 1)
    took(send1.at[:, pl.ds(0, (owners - 1) * capacity)], s1_send)
    took(send2.at[:, pl.ds(0, (reps - 1) * quota)], s2_send)
    took(meta_recv1.at[pl.ds(0, owners - 1)], m1_send)
    took(meta_recv2.at[pl.ds(0, reps - 1)], m2_send)


def join_kernel(
    meta_ref, feats, tsdf_hbm, oldw_hbm, new_tsdf_hbm, new_weight_hbm,
    acc, tsdf_ref, oldw_ref, new_tsdf_ref, new_weight_ref, sems,
):
    f32, bf16, i32 = jnp.float32, jnp.bfloat16, jnp.int32
    blocks, channels, cells = tsdf_ref.shape
    planes = channels + 1
    copies = [
        pltpu.make_async_copy(tsdf_hbm, tsdf_ref, sems.at[0]),
        pltpu.make_async_copy(oldw_hbm, oldw_ref, sems.at[1]),
    ]
    copies[0].start()
    copies[1].start()
    groups = feats.shape[0] // 8 // UNROLL
    acc[...] = jnp.zeros(acc.shape, f32)
    lower_ids = lax.broadcasted_iota(i32, (LOWERS, LANES), 0).astype(f32).astype(bf16)
    upper_ids = lax.broadcasted_iota(i32, (UPPERS, LANES), 0).astype(f32)
    empty = jnp.zeros((planes * UPPERS, LANES), f32)

    def add_groups(rows):
        for g, u in [(row, u) for row in rows for u in range(0, UNROLL, 2)]:
            rights, lefts, places = [], [], []
            for v in range(2):
                base = meta_ref[g, u + v]
                places.append(meta_ref[groups + g, u + v])
                lower = feats[pl.ds(base + 5, 1), :].astype(bf16)
                upper = feats[pl.ds(base + 6, 1), :]
                rights.append(jnp.where(lower_ids == lower, bf16(1), bf16(0)))
                hit = upper_ids == upper
                lefts.append(
                    jnp.concatenate(
                        [jnp.where(hit, feats[pl.ds(base + c, 1), :], 0.0) for c in range(planes)],
                        axis=0,
                    )
                )
            left = jnp.concatenate(
                [
                    jnp.concatenate([lefts[0], empty], axis=0),
                    jnp.concatenate([empty, lefts[1]], axis=0),
                ],
                axis=1,
            ).astype(bf16)
            both = lax.dot_general(
                left, jnp.concatenate(rights, axis=1), NT, preferred_element_type=f32
            )
            for v in range(2):
                acc[places[v], :, :LOWERS] += both[v * planes * UPPERS : (v + 1) * planes * UPPERS]

    filled = lax.div(meta_ref[2 * groups, 0] + (UNROLL - 1), UNROLL)
    pl.loop(0, lax.div(filled, 2))(lambda g: add_groups((2 * g, 2 * g + 1)))
    pl.when(lax.rem(filled, 2) == 1)(lambda: add_groups((filled - 1,)))

    copies[0].wait()
    copies[1].wait()
    lane = lax.broadcasted_iota(i32, (8, LANES), 1)

    @pl.loop(0, blocks // 8)
    def _(b8):
        base = pl.multiple_of(b8 * 8, 8)
        for h in range(cells // LANES):
            span = slice(h * LANES, (h + 1) * LANES)
            weights = oldw_ref[pl.ds(base, 8), span]
            news = []
            for i in range(8):
                even = acc[base + i, pl.ds(2 * h, planes, stride=UPPERS), :]
                odd = acc[base + i, pl.ds(2 * h + 1, planes, stride=UPPERS), :]
                sums = jnp.where(lane[:planes] < LOWERS, even, pltpu.roll(odd, LOWERS, 1))
                weight = weights[i : i + 1]
                total = weight + sums[:1]
                news.append(total)
                new_tsdf_ref[base + i, :, span] = (
                    weight * tsdf_ref[base + i, :, span] + sums[1:]
                ) / total
            new_weight_ref[pl.ds(base, 8), span] = jnp.concatenate(news, axis=0)
        part = pl.ds(base, 8)
        pltpu.make_async_copy(new_tsdf_ref.at[part], new_tsdf_hbm.at[part], sems.at[0]).start()
        pltpu.make_async_copy(new_weight_ref.at[part], new_weight_hbm.at[part], sems.at[1]).start()

    pltpu.make_async_copy(new_tsdf_ref, new_tsdf_hbm, sems.at[0]).wait()
    pltpu.make_async_copy(new_weight_ref, new_weight_hbm, sems.at[1]).wait()


def join_call(meta, feats, old_tsdf, old_weight):
    blocks, channels, cells = old_tsdf.shape
    vmem = pl.BlockSpec(memory_space=pltpu.VMEM)
    smem = pl.BlockSpec(memory_space=pltpu.SMEM)
    hbm = pl.BlockSpec(memory_space=pl.ANY)
    return pl.pallas_call(
        join_kernel,
        out_shape=(
            jax.ShapeDtypeStruct(old_tsdf.shape, jnp.float32),
            jax.ShapeDtypeStruct(old_weight.shape, jnp.float32),
        ),
        in_specs=[smem, vmem, hbm, hbm],
        out_specs=(hbm, hbm),
        scratch_shapes=[
            pltpu.VMEM((blocks + 1, (channels + 1) * UPPERS, LANES), jnp.float32),
            pltpu.VMEM(old_tsdf.shape, jnp.float32),
            pltpu.VMEM(old_weight.shape, jnp.float32),
            pltpu.VMEM(old_tsdf.shape, jnp.float32),
            pltpu.VMEM(old_weight.shape, jnp.float32),
            pltpu.SemaphoreType.DMA((2,)),
        ],
        name="join",
    )(
        pltpu.with_memory_space_constraint(meta, pltpu.SMEM),
        pltpu.with_memory_space_constraint(feats, pltpu.VMEM),
        old_tsdf,
        old_weight,
    )


def exchange_call(
    owners, reps, bin_blocks, send_counts, voxel_index, point_sdf, point_weight, point_color,
    owner_table,
):
    bins = voxel_index.shape[0]
    capacity = 2 * bins // owners
    slots = owners * capacity
    table = owner_table.reshape(-1, LANES)
    vmem = pl.BlockSpec(memory_space=pltpu.VMEM)
    smem = pl.BlockSpec(memory_space=pltpu.SMEM)
    dma = pltpu.SemaphoreType.DMA
    listing = (2 * (slots // UNROLL) + 8, LANES)
    return pl.pallas_call(
        lambda *refs: exchange_kernel(owners, reps, OWN // reps, *refs),
        out_shape=(
            pltpu.VMEM((8 * slots, LANES), jnp.float32),
            pltpu.SMEM(listing, jnp.int32),
        ),
        in_specs=[pl.BlockSpec(memory_space=pl.ANY)] * 7,
        out_specs=(vmem, smem),
        scratch_shapes=[
            pltpu.VMEM((PLANES, slots, LANES), jnp.bfloat16),
            pltpu.VMEM((PLANES, slots, LANES), jnp.bfloat16),
            pltpu.VMEM((PLANES, slots, LANES), jnp.bfloat16),
            pltpu.VMEM((PLANES, slots, LANES), jnp.bfloat16),
            pltpu.VMEM((slots, slots), jnp.bfloat16),
            pltpu.VMEM((slots // LANES, 8, LANES), jnp.float32),
            pltpu.VMEM((owners, 8, LANES), jnp.float32),
            pltpu.VMEM((reps, 8, LANES), jnp.float32),
            pltpu.VMEM((reps, 8, LANES), jnp.float32),
            pltpu.VMEM(listing, jnp.int32),
            dma,
            dma((PLANES,)),
            dma,
            dma,
            dma,
            dma((2,)),
            dma,
            dma,
            pltpu.SMEM(send_counts.shape, jnp.int32),
            pltpu.VMEM((1, bins), jnp.int32),
            pltpu.VMEM(table.shape, jnp.int32),
            pltpu.VMEM(voxel_index.shape, jnp.int32),
            pltpu.VMEM(point_sdf.shape, jnp.bfloat16),
            pltpu.VMEM(point_weight.shape, jnp.bfloat16),
            pltpu.VMEM((COLORS, bins, LANES), jnp.bfloat16),
            dma((7,)),
        ],
        compiler_params=pltpu.CompilerParams(collective_id=0, has_side_effects=True),
        name="exchange",
    )(
        send_counts,
        bin_blocks.reshape(1, bins),
        table,
        voxel_index,
        point_sdf,
        point_weight,
        jnp.transpose(point_color, (1, 0, 2)),
    )


def joined(
    bin_blocks,
    send_counts,
    voxel_index,
    point_sdf,
    point_weight,
    point_color,
    owner_table,
    old_tsdf,
    old_weight,
):
    owners, reps = lax.axis_size("owner"), lax.axis_size("rep")
    bins, points = voxel_index.shape
    capacity = 2 * bins // owners
    quota = 2 * bins // reps
    if owners != 8 or reps != 4 or bins != 256 or points != LANES:
        return local(
            bin_blocks, send_counts, voxel_index, point_sdf, point_weight, point_color,
            owner_table, old_tsdf, old_weight,
        )
    feats, meta = exchange_call(
        owners, reps, bin_blocks, send_counts, voxel_index, point_sdf, point_weight, point_color,
        owner_table,
    )
    return join_call(meta, feats, old_tsdf, old_weight)


def solution(mesh):
    placed = (
        P(("owner", "rep")),
        P(("owner", "rep"), None),
        P(("owner", "rep"), None),
        P(("owner", "rep"), None),
        P(("owner", "rep"), None),
        P(("owner", "rep"), None, None),
        P(),
        P(("owner", "rep"), None, None),
        P(("owner", "rep"), None),
    )
    return jax.shard_map(
        joined,
        mesh=mesh,
        in_specs=placed,
        out_specs=(P(("owner", "rep"), None, None), P(("owner", "rep"), None)),
        check_vma=False,
    )
```

```python
import math

import jax
import jax.numpy as jnp
from jax import lax
from jax.experimental import pallas as pl
from jax.experimental.pallas import tpu as pltpu
from jax.sharding import PartitionSpec as P

OWN = 256
VA = 8
VB = 64


def accumulate(feature_list, voxels, block_rows, block_total):
    slot_count, points = voxels.shape
    group_size = math.gcd(slot_count, 128)
    group_count = slot_count // group_size
    channels = sum_channels(feature_list)
    grouped = tuple((f.reshape((group_count, group_size) + f.shape[1:]) for f in feature_list))
    voxel_groups = voxels.reshape(group_count, group_size, points)
    block_groups = jnp.maximum(block_rows, 0).reshape(group_count, group_size)
    upper_ids = jnp.arange(VA, dtype=jnp.int32)
    lower_ids = jnp.arange(VB, dtype=jnp.int32)

    def fold_group(running, pieces):
        feature_parts, voxel_rows, block_ids = pieces
        features_group = jnp.concatenate(list(feature_parts), axis=1)
        upper_part = voxel_rows // VB
        lower_part = voxel_rows % VB
        chosen = upper_part[:, None, :] == upper_ids[None, :, None]
        left_side = jnp.where(
            chosen[:, None], features_group[:, :, None, :], jnp.zeros((), jnp.bfloat16)
        )
        left_side = left_side.reshape(group_size, channels * VA, points)
        right_side = (lower_part[:, :, None] == lower_ids[None, None, :]).astype(jnp.bfloat16)
        slot_grids = jnp.einsum(
            "gkp,gpb->gkb", left_side, right_side, preferred_element_type=jnp.float32
        )
        slot_grids = slot_grids.reshape(group_size, channels, VA * VB)
        return (running.at[block_ids].add(slot_grids), None)

    running_start = jnp.zeros((block_total, channels, VA * VB), jnp.float32)
    running_end, _ = lax.scan(fold_group, running_start, (grouped, voxel_groups, block_groups))
    return running_end


def sum_channels(feature_list):
    total_channels = 0
    for member in feature_list:
        total_channels = total_channels + member.shape[1]
    return total_channels


def local(
    bin_blocks,
    send_counts,
    voxel_index,
    point_sdf,
    point_weight,
    point_color,
    owner_table,
    old_tsdf,
    old_weight,
):
    owners = lax.axis_size("owner")
    bin_count = bin_blocks.shape[0]
    capacity = 2 * bin_count // owners
    slot_count = owners * capacity
    counts = send_counts[0]
    starts = jnp.cumsum(counts) - counts
    slot_ids = jnp.arange(slot_count, dtype=jnp.int32)
    target = slot_ids // capacity
    position = slot_ids % capacity
    active = position < counts[target]
    source = jnp.clip(starts[target] + position, 0, bin_count - 1)
    blocks_sent = jnp.where(active, owner_table[bin_blocks[source]] % OWN, -1)
    weight = jnp.where(active[:, None], point_weight[source], jnp.zeros((), jnp.bfloat16))
    wide_weight = weight.astype(jnp.float32)
    weighted_sdf = (wide_weight * point_sdf[source].astype(jnp.float32)).astype(jnp.bfloat16)
    geometry = jnp.stack([weight, weighted_sdf], axis=1)
    colors = (wide_weight[:, None, :] * point_color[source].astype(jnp.float32)).astype(
        jnp.bfloat16
    )
    voxels = voxel_index[source]
    replicas = lax.axis_size("rep")
    share = OWN // replicas
    arrived_geometry, arrived_colors, arrived_voxels, arrived_blocks = (
        lax.all_to_all(geometry, "owner", split_axis=0, concat_axis=0, tiled=True),
        lax.all_to_all(colors, "owner", split_axis=0, concat_axis=0, tiled=True),
        lax.all_to_all(voxels, "owner", split_axis=0, concat_axis=0, tiled=True),
        lax.all_to_all(blocks_sent, "owner", split_axis=0, concat_axis=0, tiled=True),
    )
    quota = 2 * bin_count // replicas
    live = arrived_blocks >= 0
    quarter = jnp.where(live, arrived_blocks // share, 0)
    quarter_ids = jnp.arange(replicas, dtype=jnp.int32)
    member = (live[:, None] & (quarter[:, None] == quarter_ids[None, :])).astype(jnp.int32)
    rank = jnp.sum((jnp.cumsum(member, axis=0) - member) * member, axis=1)
    outgoing_slots = replicas * quota
    destination = jnp.where(live, quarter * quota + rank, outgoing_slots).astype(jnp.int32)
    arrived_ids = jnp.arange(arrived_blocks.shape[0], dtype=jnp.int32)
    picked = jnp.zeros((outgoing_slots,), jnp.int32).at[destination].set(arrived_ids, mode="drop")
    filled = jnp.zeros((outgoing_slots,), jnp.bool_).at[destination].set(True, mode="drop")
    send_geometry = jnp.where(
        filled[:, None, None], arrived_geometry[picked], jnp.zeros((), jnp.bfloat16)
    )
    send_colors = jnp.where(
        filled[:, None, None], arrived_colors[picked], jnp.zeros((), jnp.bfloat16)
    )
    send_voxels = arrived_voxels[picked]
    send_places = jnp.where(filled, arrived_blocks[picked] % share, -1).astype(jnp.int32)
    final_geometry, final_colors, final_voxels, final_places = (
        lax.all_to_all(send_geometry, "rep", split_axis=0, concat_axis=0, tiled=True),
        lax.all_to_all(send_colors, "rep", split_axis=0, concat_axis=0, tiled=True),
        lax.all_to_all(send_voxels, "rep", split_axis=0, concat_axis=0, tiled=True),
        lax.all_to_all(send_places, "rep", split_axis=0, concat_axis=0, tiled=True),
    )
    cell_sums = accumulate((final_geometry, final_colors), final_voxels, final_places, share)
    geometry_share = cell_sums[:, :2]
    color_share = cell_sums[:, 2:]
    new_weight = old_weight + geometry_share[:, 0]
    joined_sdf = (old_weight * old_tsdf[:, 0] + geometry_share[:, 1]) / new_weight
    joined_color = (old_weight[:, None, :] * old_tsdf[:, 1:] + color_share) / new_weight[:, None, :]
    new_tsdf = jnp.concatenate([joined_sdf[:, None, :], joined_color], axis=1)
    return (new_tsdf, new_weight)


PLANES = 6
COLORS = 3
LANES = 128
LOG = 7
UPPERS = 8
LOWERS = 64
UNROLL = 64
FAR = (4, 5, 6, 7)
NEAR = (2, 3, 1)
LAG = 2
MESH = pl.DeviceIdType.MESH
NT = (((1,), (1,)), ((), ()))
NN = (((1,), (0,)), ((), ()))


def mirrored(index, bits):
    bit = 1
    while bit <= bits:
        if bits & bit:
            index = index + bit * (1 - 2 * lax.rem(lax.div(index, bit), 2))
        bit *= 2
    return index


def exchange_kernel(
    owners, reps, share,
    counts_hbm, bins_hbm, table_hbm, voxel_hbm, sdf_hbm, weight_hbm, color_hbm,
    feats_ref, meta_ref,
    send1, recv1, send2, final, pick2_ref, meta_send1, meta_recv1, meta_send2, meta_recv2, listed,
    s1_send, s1_recv, m1_send, m1_recv, s2_send, s2_recv, m2_send, m2_recv,
    counts_ref, bins_ref, table_ref, voxel_ref, sdf_ref, weight_ref, color_ref, load_sem,
):
    f32, bf16, i32 = jnp.float32, jnp.bfloat16, jnp.int32
    bins = voxel_ref.shape[0]
    capacity = 2 * bins // owners
    slots = owners * capacity
    quota = 2 * bins // reps
    me = lax.axis_index("owner")
    my_rep = lax.axis_index("rep")
    barrier = pltpu.get_barrier_semaphore()
    for k in FAR + NEAR:
        pl.semaphore_signal(barrier, inc=1, device_id=(mirrored(me, k), my_rep), device_id_type=MESH)
    for k in range(1, reps):
        pl.semaphore_signal(
            barrier, inc=1, device_id=(me, mirrored(my_rep, k)), device_id_type=MESH
        )

    loads = [
        pltpu.make_async_copy(source, target, load_sem.at[i])
        for i, (source, target) in enumerate(
            (
                (counts_hbm, counts_ref),
                (voxel_hbm, voxel_ref),
                (bins_hbm, bins_ref),
                (table_hbm, table_ref),
                (weight_hbm, weight_ref),
                (sdf_hbm, sdf_ref),
                (color_hbm, color_ref),
            )
        )
    ]
    for load in loads:
        load.start()

    def owner_copy(p, partner):
        return pltpu.make_async_remote_copy(
            src_ref=send1.at[p, pl.ds(pl.multiple_of(partner * capacity, capacity), capacity)],
            dst_ref=recv1.at[p, pl.ds(pl.multiple_of(me * capacity, capacity), capacity)],
            send_sem=s1_send,
            recv_sem=s1_recv.at[p],
            device_id=(partner, my_rep),
            device_id_type=MESH,
        )

    def took(bytes_of, semaphore):
        pltpu.make_async_copy(bytes_of, bytes_of, semaphore).wait()

    def send_copy(p, partner):
        owner_copy(p, partner).start()

    def owner_meta(k):
        partner = mirrored(me, k)
        return pltpu.make_async_remote_copy(
            src_ref=meta_send1.at[lax.div(partner, 2)],
            dst_ref=meta_recv1.at[me],
            send_sem=m1_send,
            recv_sem=m1_recv,
            device_id=(partner, my_rep),
            device_id_type=MESH,
        )

    def quarter_rows(q):
        return pl.ds(pl.multiple_of(q * quota, quota), quota)

    def rep_copy(p, k):
        partner = mirrored(my_rep, k)
        return pltpu.make_async_remote_copy(
            src_ref=send2.at[p, quarter_rows(partner)],
            dst_ref=final.at[p, quarter_rows(my_rep)],
            send_sem=s2_send,
            recv_sem=s2_recv.at[p // (PLANES - 1)],
            device_id=(me, partner),
            device_id_type=MESH,
        )

    def rep_meta(k):
        partner = mirrored(my_rep, k)
        return pltpu.make_async_remote_copy(
            src_ref=meta_send2.at[partner],
            dst_ref=meta_recv2.at[my_rep],
            send_sem=m2_send,
            recv_sem=m2_recv,
            device_id=(me, partner),
            device_id_type=MESH,
        )

    lane_bin = lax.broadcasted_iota(i32, (capacity, bins), 1)
    row_slot = lax.broadcasted_iota(i32, (capacity, bins), 0)
    loads[0].wait()
    picks = []
    start = jnp.int32(0)
    for t in range(owners):
        count = counts_ref[0, t]
        hit = (lane_bin == row_slot + start) & (row_slot < count)
        picks.append(jnp.where(hit, 1.0, 0.0).astype(bf16))
        start = start + count
    pick1 = jnp.concatenate(picks, axis=0)

    half = owners // 2
    upper_half = lax.div(me, half)
    across = (1 - upper_half) * (me + half)
    far = [mirrored(across, j) for j in range(half)]
    near = [mirrored(me, k) for k in NEAR]

    def send_plane(p, data):
        send1[p] = lax.dot_general(pick1, data, NN, preferred_element_type=f32).astype(bf16)
        if p == 0:
            pl.semaphore_wait(barrier, owners + reps - 2)
        send_copy(p, far[0])
        for partner in near:
            send_copy(p, partner)
        if p == 0:
            for partner in far[1:]:
                send_copy(p, partner)
        elif p >= LAG:
            for partner in far[1:]:
                send_copy(p - LAG + 1, partner)

    loads[1].wait()
    send_plane(0, (voxel_ref[...] - 256).astype(f32).astype(bf16))

    loads[2].wait()
    loads[3].wait()
    ids = bins_ref[...]
    low = lax.broadcasted_iota(i32, (LANES, bins), 0) == (ids & (LANES - 1))
    rows = table_ref.shape[0]
    table = (table_ref[...] & (OWN - 1)).astype(f32).astype(bf16)
    looked = lax.dot_general(
        table, jnp.where(low, 1.0, 0.0).astype(bf16), NN, preferred_element_type=f32
    )
    high = lax.broadcasted_iota(i32, (rows, bins), 0) == lax.shift_right_logical(ids, LOG)
    place = jnp.sum(jnp.where(high, looked, 0.0), axis=0, keepdims=True) + 1.0
    place = jnp.broadcast_to(place, (8, bins)).astype(bf16)
    sent_places = lax.dot_general(place, pick1, NT, preferred_element_type=f32)
    for t in range(slots // LANES):
        meta_send1[t] = sent_places[:, t * LANES : (t + 1) * LANES]
    for k in FAR + NEAR:
        owner_meta(k).start()

    loads[4].wait()
    weight = weight_ref[...]
    wide = weight.astype(f32)
    send_plane(1, weight)
    loads[5].wait()
    send_plane(2, (wide * sdf_ref[...].astype(f32)).astype(bf16))
    loads[6].wait()
    for c in range(COLORS):
        send_plane(3 + c, (wide * color_ref[c].astype(f32)).astype(bf16))

    for p in range(PLANES - LAG + 1, PLANES):
        for partner in far[1:]:
            send_copy(p, partner)

    mine = pl.ds(pl.multiple_of(me * capacity, capacity), capacity)
    for p in range(PLANES):
        recv1[p, mine] = send1[p, mine]
    meta_recv1[me] = meta_send1[lax.div(me, 2)]

    before = lax.broadcasted_iota(i32, (slots, slots), 0) < lax.broadcasted_iota(
        i32, (slots, slots), 1
    )
    before = jnp.where(before, 1.0, 0.0).astype(bf16)
    took(meta_recv1.at[pl.ds(0, owners - 1)], m1_recv)
    lane = lax.broadcasted_iota(i32, (8, LANES), 1)
    even = lax.rem(me, 2) == 0
    pieces = []
    for pair in range(owners // 2):
        first, second = meta_recv1[2 * pair], meta_recv1[2 * pair + 1]
        first = jnp.where(even, first, pltpu.roll(first, capacity, 1))
        second = jnp.where(even, pltpu.roll(second, capacity, 1), second)
        pieces.append(jnp.where(lane < capacity, first, second))
    arrived = jnp.concatenate(pieces, axis=1)
    arrived_id = arrived.astype(i32) - 1
    quarter = jnp.where(arrived_id < 0, -1, lax.div(arrived_id, share))
    member = lax.broadcasted_iota(i32, (8, slots), 0) == quarter
    ranks = lax.dot_general(
        jnp.where(member, 1.0, 0.0).astype(bf16), before, NN, preferred_element_type=f32
    )
    rank = jnp.sum(jnp.where(member, ranks, 0.0), axis=0, keepdims=True).astype(i32)
    goal = jnp.where(arrived_id[:1] < 0, -1, quarter[:1] * quota + rank)
    pick2 = jnp.where(lax.broadcasted_iota(i32, (reps * quota, slots), 0) == goal, 1.0, 0.0)
    pick2 = pick2.astype(bf16)
    pick2_ref[...] = pick2
    final_place = jnp.where(arrived_id < 0, 0, lax.rem(arrived_id, share) + 1).astype(f32).astype(bf16)
    final_place = lax.dot_general(final_place, pick2, NT, preferred_element_type=f32)
    for q in range(reps):
        meta_send2[q] = final_place[:, q * quota : (q + 1) * quota]
    for k in range(1, reps):
        rep_meta(k).start()
    meta_recv2[my_rep] = meta_send2[my_rep]

    def relay(p):
        took(recv1.at[p, pl.ds(0, (owners - 1) * capacity)], s1_recv.at[p])
        data = recv1[p]
        side = lax.div(my_rep, 2)
        for half, partners in ((1 - side, (2, 3)), (side, (1,))):
            rows = pl.ds(pl.multiple_of(half * 2 * quota, 2 * quota), 2 * quota)
            send2[p, rows] = lax.dot_general(
                pick2_ref[rows], data, NN, preferred_element_type=f32
            ).astype(bf16)
            for k in partners:
                rep_copy(p, k).start()
        final[p, quarter_rows(my_rep)] = send2[p, quarter_rows(my_rep)]

    def land(p):
        data = final[p].astype(f32)
        if p > 0:
            feats_ref[pl.ds(p - 1, slots, stride=8), :] = data
        else:
            voxel = data.astype(i32) + 256
            feats_ref[pl.ds(5, slots, stride=8), :] = (voxel & (LOWERS - 1)).astype(f32)
            feats_ref[pl.ds(6, slots, stride=8), :] = lax.shift_right_logical(voxel, 6).astype(f32)

    def list_slots():
        took(meta_recv2.at[pl.ds(0, reps - 1)], m2_recv)
        lane = lax.broadcasted_iota(i32, (8, LANES), 1)
        row = lax.broadcasted_iota(i32, (8, LANES), 0)
        targets, values = [], []
        start = jnp.zeros((1, 1), f32)
        for r in range(reps):
            tile = meta_recv2[r]
            live = tile[:1] > 0
            targets.append(jnp.where(live, lane[:1].astype(f32) + start, -1.0))
            values.append(
                jnp.where(row == 0, float(r), jnp.where(row == 1, lane.astype(f32), tile))
            )
            start = start + jnp.sum(jnp.where(live, 1.0, 0.0), axis=1, keepdims=True)
        target = jnp.concatenate(targets, axis=1).astype(i32)
        chosen = lax.broadcasted_iota(i32, (slots, slots), 0) == target
        found = lax.dot_general(
            jnp.concatenate(values, axis=1).astype(bf16),
            jnp.where(chosen, 1.0, 0.0).astype(bf16),
            NT, preferred_element_type=f32,
        )
        base = ((found[:1] * float(quota) + found[1:2]) * 8.0).astype(i32)
        spot = found[2:3].astype(i32)
        spot = jnp.where(spot > 0, spot - 1, share)
        groups = slots // UNROLL
        for g in range(groups):
            part = pl.ds((g * UNROLL) // LANES * LANES, LANES)
            shift = (LANES - (g * UNROLL) % LANES) % LANES
            for source, place in ((base, g), (spot, groups + g)):
                tile = source[:, part.start : part.start + LANES]
                if shift:
                    tile = pltpu.roll(jnp.broadcast_to(tile, (8, LANES)), shift, 1)[:1]
                listed[place : place + 1] = tile
        listed[2 * groups : 2 * groups + 1] = jnp.broadcast_to(start.astype(i32), (1, LANES))
        copy = pltpu.make_async_copy(listed, meta_ref, load_sem.at[0])
        copy.start()
        return copy

    for p in range(PLANES):
        relay(p)
        if p == 3:
            copy = list_slots()
    copy.wait()
    took(final.at[pl.ds(0, PLANES - 1), pl.ds(0, (reps - 1) * quota)], s2_recv.at[0])
    for p in range(PLANES - 1):
        land(p)
    took(final.at[PLANES - 1, pl.ds(0, (reps - 1) * quota)], s2_recv.at[1])
    land(PLANES - 1)
    took(send1.at[:, pl.ds(0, (owners - 1) * capacity)], s1_send)
    took(send2.at[:, pl.ds(0, (reps - 1) * quota)], s2_send)
    took(meta_recv1.at[pl.ds(0, owners - 1)], m1_send)
    took(meta_recv2.at[pl.ds(0, reps - 1)], m2_send)


def join_kernel(
    meta_ref, feats, tsdf_hbm, oldw_hbm, new_tsdf_hbm, new_weight_hbm,
    acc, tsdf_ref, oldw_ref, new_tsdf_ref, new_weight_ref, sems,
):
    f32, bf16, i32 = jnp.float32, jnp.bfloat16, jnp.int32
    blocks, channels, cells = tsdf_ref.shape
    planes = channels + 1
    copies = [
        pltpu.make_async_copy(tsdf_hbm, tsdf_ref, sems.at[0]),
        pltpu.make_async_copy(oldw_hbm, oldw_ref, sems.at[1]),
    ]
    copies[0].start()
    copies[1].start()
    groups = feats.shape[0] // 8 // UNROLL
    acc[...] = jnp.zeros(acc.shape, f32)
    lower_ids = lax.broadcasted_iota(i32, (LOWERS, LANES), 0).astype(f32).astype(bf16)
    upper_ids = lax.broadcasted_iota(i32, (UPPERS, LANES), 0).astype(f32)
    empty = jnp.zeros((planes * UPPERS, LANES), f32)

    def add_groups(rows):
        for g, u in [(row, u) for row in rows for u in range(0, UNROLL, 2)]:
            rights, lefts, places = [], [], []
            for v in range(2):
                base = meta_ref[g, u + v]
                places.append(meta_ref[groups + g, u + v])
                lower = feats[pl.ds(base + 5, 1), :].astype(bf16)
                upper = feats[pl.ds(base + 6, 1), :]
                rights.append(jnp.where(lower_ids == lower, bf16(1), bf16(0)))
                hit = upper_ids == upper
                lefts.append(
                    jnp.concatenate(
                        [jnp.where(hit, feats[pl.ds(base + c, 1), :], 0.0) for c in range(planes)],
                        axis=0,
                    )
                )
            left = jnp.concatenate(
                [
                    jnp.concatenate([lefts[0], empty], axis=0),
                    jnp.concatenate([empty, lefts[1]], axis=0),
                ],
                axis=1,
            ).astype(bf16)
            both = lax.dot_general(
                left, jnp.concatenate(rights, axis=1), NT, preferred_element_type=f32
            )
            for v in range(2):
                acc[places[v], :, :LOWERS] += both[v * planes * UPPERS : (v + 1) * planes * UPPERS]

    filled = lax.div(meta_ref[2 * groups, 0] + (UNROLL - 1), UNROLL)
    pl.loop(0, lax.div(filled, 2))(lambda g: add_groups((2 * g, 2 * g + 1)))
    pl.when(lax.rem(filled, 2) == 1)(lambda: add_groups((filled - 1,)))

    copies[0].wait()
    copies[1].wait()
    lane = lax.broadcasted_iota(i32, (8, LANES), 1)

    @pl.loop(0, blocks // 8)
    def _(b8):
        base = pl.multiple_of(b8 * 8, 8)
        for h in range(cells // LANES):
            span = slice(h * LANES, (h + 1) * LANES)
            weights = oldw_ref[pl.ds(base, 8), span]
            news = []
            for i in range(8):
                even = acc[base + i, pl.ds(2 * h, planes, stride=UPPERS), :]
                odd = acc[base + i, pl.ds(2 * h + 1, planes, stride=UPPERS), :]
                sums = jnp.where(lane[:planes] < LOWERS, even, pltpu.roll(odd, LOWERS, 1))
                weight = weights[i : i + 1]
                total = weight + sums[:1]
                news.append(total)
                new_tsdf_ref[base + i, :, span] = (
                    weight * tsdf_ref[base + i, :, span] + sums[1:]
                ) / total
            new_weight_ref[pl.ds(base, 8), span] = jnp.concatenate(news, axis=0)
        part = pl.ds(base, 8)
        pltpu.make_async_copy(new_tsdf_ref.at[part], new_tsdf_hbm.at[part], sems.at[0]).start()
        pltpu.make_async_copy(new_weight_ref.at[part], new_weight_hbm.at[part], sems.at[1]).start()

    pltpu.make_async_copy(new_tsdf_ref, new_tsdf_hbm, sems.at[0]).wait()
    pltpu.make_async_copy(new_weight_ref, new_weight_hbm, sems.at[1]).wait()


def join_call(meta, feats, old_tsdf, old_weight):
    blocks, channels, cells = old_tsdf.shape
    vmem = pl.BlockSpec(memory_space=pltpu.VMEM)
    smem = pl.BlockSpec(memory_space=pltpu.SMEM)
    hbm = pl.BlockSpec(memory_space=pl.ANY)
    return pl.pallas_call(
        join_kernel,
        out_shape=(
            jax.ShapeDtypeStruct(old_tsdf.shape, jnp.float32),
            jax.ShapeDtypeStruct(old_weight.shape, jnp.float32),
        ),
        in_specs=[smem, vmem, hbm, hbm],
        out_specs=(hbm, hbm),
        scratch_shapes=[
            pltpu.VMEM((blocks + 1, (channels + 1) * UPPERS, LANES), jnp.float32),
            pltpu.VMEM(old_tsdf.shape, jnp.float32),
            pltpu.VMEM(old_weight.shape, jnp.float32),
            pltpu.VMEM(old_tsdf.shape, jnp.float32),
            pltpu.VMEM(old_weight.shape, jnp.float32),
            pltpu.SemaphoreType.DMA((2,)),
        ],
        name="join",
    )(
        pltpu.with_memory_space_constraint(meta, pltpu.SMEM),
        pltpu.with_memory_space_constraint(feats, pltpu.VMEM),
        old_tsdf,
        old_weight,
    )


def exchange_call(
    owners, reps, bin_blocks, send_counts, voxel_index, point_sdf, point_weight, point_color,
    owner_table,
):
    bins = voxel_index.shape[0]
    capacity = 2 * bins // owners
    slots = owners * capacity
    table = owner_table.reshape(-1, LANES)
    vmem = pl.BlockSpec(memory_space=pltpu.VMEM)
    smem = pl.BlockSpec(memory_space=pltpu.SMEM)
    dma = pltpu.SemaphoreType.DMA
    listing = (2 * (slots // UNROLL) + 8, LANES)
    return pl.pallas_call(
        lambda *refs: exchange_kernel(owners, reps, OWN // reps, *refs),
        out_shape=(
            pltpu.VMEM((8 * slots, LANES), jnp.float32),
            pltpu.SMEM(listing, jnp.int32),
        ),
        in_specs=[pl.BlockSpec(memory_space=pl.ANY)] * 7,
        out_specs=(vmem, smem),
        scratch_shapes=[
            pltpu.VMEM((PLANES, slots, LANES), jnp.bfloat16),
            pltpu.VMEM((PLANES, slots, LANES), jnp.bfloat16),
            pltpu.VMEM((PLANES, slots, LANES), jnp.bfloat16),
            pltpu.VMEM((PLANES, slots, LANES), jnp.bfloat16),
            pltpu.VMEM((slots, slots), jnp.bfloat16),
            pltpu.VMEM((slots // LANES, 8, LANES), jnp.float32),
            pltpu.VMEM((owners, 8, LANES), jnp.float32),
            pltpu.VMEM((reps, 8, LANES), jnp.float32),
            pltpu.VMEM((reps, 8, LANES), jnp.float32),
            pltpu.VMEM(listing, jnp.int32),
            dma,
            dma((PLANES,)),
            dma,
            dma,
            dma,
            dma((2,)),
            dma,
            dma,
            pltpu.SMEM(send_counts.shape, jnp.int32),
            pltpu.VMEM((1, bins), jnp.int32),
            pltpu.VMEM(table.shape, jnp.int32),
            pltpu.VMEM(voxel_index.shape, jnp.int32),
            pltpu.VMEM(point_sdf.shape, jnp.bfloat16),
            pltpu.VMEM(point_weight.shape, jnp.bfloat16),
            pltpu.VMEM((COLORS, bins, LANES), jnp.bfloat16),
            dma((7,)),
        ],
        compiler_params=pltpu.CompilerParams(collective_id=0, has_side_effects=True),
        name="exchange",
    )(
        send_counts,
        bin_blocks.reshape(1, bins),
        table,
        voxel_index,
        point_sdf,
        point_weight,
        jnp.transpose(point_color, (1, 0, 2)),
    )


def joined(
    bin_blocks,
    send_counts,
    voxel_index,
    point_sdf,
    point_weight,
    point_color,
    owner_table,
    old_tsdf,
    old_weight,
):
    owners, reps = lax.axis_size("owner"), lax.axis_size("rep")
    bins, points = voxel_index.shape
    capacity = 2 * bins // owners
    quota = 2 * bins // reps
    if owners != 8 or reps != 4 or bins != 256 or points != LANES:
        return local(
            bin_blocks, send_counts, voxel_index, point_sdf, point_weight, point_color,
            owner_table, old_tsdf, old_weight,
        )
    feats, meta = exchange_call(
        owners, reps, bin_blocks, send_counts, voxel_index, point_sdf, point_weight, point_color,
        owner_table,
    )
    return join_call(meta, feats, old_tsdf, old_weight)


def solution(mesh):
    placed = (
        P(("owner", "rep")),
        P(("owner", "rep"), None),
        P(("owner", "rep"), None),
        P(("owner", "rep"), None),
        P(("owner", "rep"), None),
        P(("owner", "rep"), None, None),
        P(),
        P(("owner", "rep"), None, None),
        P(("owner", "rep"), None),
    )
    return jax.shard_map(
        joined,
        mesh=mesh,
        in_specs=placed,
        out_specs=(P(("owner", "rep"), None, None), P(("owner", "rep"), None)),
        check_vma=False,
    )
```
